32 devices in a mesh: parts: 2 (over y), row: 4 (over z), col: 4 (over x, core).
Axes of the slice: x: 2, y: 2, z: 4, core: 2. Of those that a mesh axis runs over, the one named last changes fastest.
Arguments:
- state: float32 [10, 128, 512], P(None, ('parts', 'row'), 'col'), parts along dimension 1, may hold values from -5 to 5
- history: float32 [10, 128, 512], P(None, ('parts', 'row'), 'col'), parts along dimension 1, may hold values from -5 to 5
- rates: float32 [10, 10, 128, 512], P(None, None, ('parts', 'row'), 'col'), parts along dimension 2, may hold values from -2 to 2
- quadratic: float32 [10, 128, 512], P(None, ('parts', 'row'), 'col'), parts along dimension 1, may hold values from 0.1 to 1
- velocity: float32 [10, 2], replicated, may hold values from -1.5 to 1.5
- precond: float32 [10, 10, 128, 512], P(None, None, ('parts', 'row'), 'col'), parts along dimension 2, may hold values from -1 to 2, as said below
Outputs:
- updated: float32 [10, 128, 512], P(None, ('parts', 'row'), 'col'), parts along dimension 1
- lin_residual: float32 [2], P('parts'), parts along dimension 0
The draws below stay inside these ranges and needn't reach their ends.
There are 2 independent parts, one for each index of `parts`. The reference program is written for one: setup_inputs(seed, part) draws one part's arguments, and reference() takes and returns one part's arrays. A program takes and returns all parts, laid end to end along the dimension named above; an argument that names none is the same for every part. Nothing has to cross between parts.
Inputs may be any that keep to these rules, and one draw needn't show every extreme that they name: `precond`: each cell's block has diagonal entries 1 plus a spread term and independent off-diagonal entries.
All inputs are finite; a program needn't handle non-finite values.
Results may differ from the reference program's by a relative error of at most 0.00011.
Values sent between devices are 32-bit elements; how exact they have to be, the bound alone decides.
No kernel may reach another device: no remote copies, remote signals or barrier semaphores. Data moves between devices by JAX's collectives and lax.ppermute only.
A program may use at most 64 MiB of HBM per device.

```python
import jax
import jax.numpy as jnp
from jax import lax

SPECIES = 10
KRYLOV = 4
NX = 64
NY = 512


def draw_precond(key, part):
    spread = jnp.clip(0.25 * jax.random.normal(key, (SPECIES, SPECIES, NX, NY), jnp.float32), -1.0, 1.0)
    identity = jnp.eye(SPECIES, dtype=jnp.float32)[:, :, None, None]
    return identity + spread


def block_scale(own_key, shape, pieces, least, top_value):
    def one(axis_at, shards_of):
        steps = jax.random.uniform(jax.random.fold_in(jax.random.fold_in(own_key, 6), axis_at), (shards_of,), jnp.float32, least / len(pieces), top_value / len(pieces))
        return jnp.repeat(jnp.exp(steps), shape[axis_at] // shards_of).reshape((-1,) + (1,) * (len(shape) - axis_at - 1))

    loudness = one(*pieces[0])
    for cut in pieces[1:]:
        loudness = loudness * one(*cut)
    return loudness


def centred(own_key, shape, deviation, most, cuts=(), kind=jnp.bfloat16):
    gain = block_scale(own_key, shape, cuts, -0.22, 0.18) if cuts else 1.0
    drawn = jax.random.normal(own_key, shape, jnp.float32) * deviation * gain
    return jnp.minimum(jnp.maximum(drawn, -most), most).astype(kind)


def setup_inputs(seed: int = 0, part: int = 0) -> dict:
    splits = jax.random.split(jax.random.key(seed), 7)
    own_keys = jax.random.split(jax.random.fold_in(splits[6], part), 7)
    state = centred(own_keys[0], (SPECIES, NX, NY), 1.0, 5.0, ((1, 4), (2, 4)), jnp.float32)
    history = centred(own_keys[1], (SPECIES, NX, NY), 1.0, 5.0, ((1, 4), (2, 4)), jnp.float32)
    rates = centred(own_keys[2], (SPECIES, SPECIES, NX, NY), SPECIES ** -0.5, 2.0, ((2, 4), (3, 4)), jnp.float32)
    quadratic = jnp.clip(0.1 + 0.9 * jax.random.uniform(own_keys[3], (SPECIES, NX, NY), jnp.float32) ** block_scale(own_keys[3], (SPECIES, NX, NY), ((1, 4), (2, 4)), -0.2, 0.2), 0.1, 1.0)
    velocity = jnp.clip(jax.random.uniform(splits[4], (SPECIES, 2), jnp.float32, -1.5, 1.5), -1.5, 1.5)
    precond = draw_precond(jax.random.fold_in(jax.random.fold_in(splits[6], part), 71), part)
    return dict(state=state, history=history, rates=rates, quadratic=quadratic, velocity=velocity, precond=precond)


step_gamma = 0.4
tiny_eps = 1e-12

def advect(field, velocity):
    padded = jnp.pad(field, ((0, 0), (1, 1), (1, 1)))
    along_x = padded[:, 2:, 1:-1] - padded[:, :-2, 1:-1]
    along_y = padded[:, 1:-1, 2:] - padded[:, 1:-1, :-2]
    return -0.5 * (velocity[:, 0][:, None, None] * along_x + velocity[:, 1][:, None, None] * along_y)

def blockmul(matrix, field):
    return lax.optimization_barrier(jnp.sum(matrix * field[None], axis=1))

def least_squares(hessen, beta):
    width = hessen.shape[1]
    rotated = jnp.zeros((width + 1,), jnp.float32).at[0].set(beta)
    upper = hessen
    for index in range(width):
        first = upper[index, index]
        second = upper[index + 1, index]
        radius = jnp.sqrt(first * first + second * second)
        cosine = first / radius
        sine = second / radius
        row_top = cosine * upper[index] + sine * upper[index + 1]
        row_low = -sine * upper[index] + cosine * upper[index + 1]
        upper = upper.at[index].set(row_top).at[index + 1].set(row_low)
        g_top = cosine * rotated[index] + sine * rotated[index + 1]
        g_low = -sine * rotated[index] + cosine * rotated[index + 1]
        rotated = rotated.at[index].set(g_top).at[index + 1].set(g_low)
    coef = jnp.zeros((width,), jnp.float32)
    for index in reversed(range(width)):
        partial_sum = jnp.sum(upper[index, index + 1:width] * coef[index + 1:width])
        coef = coef.at[index].set((rotated[index] - partial_sum) / upper[index, index])
    return (coef, jnp.abs(rotated[width]))

def reference(state, history, rates, quadratic, velocity, precond):
    forcing = advect(state, velocity) + blockmul(rates, state) - quadratic * state * state
    rhs = -(state - history - step_gamma * forcing)

    def apply_matrix(field):
        jac = advect(field, velocity) + blockmul(rates, field) - 2.0 * quadratic * state * field
        return field - step_gamma * jac
    beta = jnp.sqrt(jnp.sum(rhs * rhs) + tiny_eps)
    basis = [rhs / beta]
    hessen = jnp.zeros((KRYLOV + 1, KRYLOV), jnp.float32)
    for index in range(KRYLOV):
        vector = apply_matrix(blockmul(precond, basis[index]))
        stacked = jnp.stack(basis)
        dots = lax.optimization_barrier(jnp.sum(stacked * vector[None], axis=(1, 2, 3)))
        vector = vector - lax.optimization_barrier(jnp.sum(dots[:, None, None, None] * stacked, axis=0))
        size_new = jnp.sqrt(jnp.sum(vector * vector) + tiny_eps)
        hessen = hessen.at[:index + 1, index].set(dots).at[index + 1, index].set(size_new)
        basis.append(vector / size_new)
    coef, lin_norm = least_squares(hessen, beta)
    combined = lax.optimization_barrier(jnp.sum(coef[:, None, None, None] * jnp.stack(basis[:KRYLOV]), axis=0))
    updated = state + blockmul(precond, combined)
    return (updated, jnp.reshape(lin_norm, (1,)))
```

```python
import functools

import jax
import jax.numpy as jnp
from jax import lax
from jax.experimental import pallas as pl
from jax.experimental.pallas import tpu as pltpu
from jax.sharding import PartitionSpec as P

KRYLOV = 4
step_gamma = 0.4
tiny_eps = 1e-12

F32 = jnp.float32
LANES = 128
VMEM = pltpu.CompilerParams(vmem_limit_bytes=48 * 1024 * 1024)


def lane_of(rows):
    return lax.broadcasted_iota(jnp.int32, (rows, LANES), 1)


def row_of(rows):
    return lax.broadcasted_iota(jnp.int32, (rows, LANES), 0)


def roll_lanes(x, shift):
    shift %= LANES
    return pltpu.roll(x, shift, 1) if shift else x


def roll_rows(x, shift):
    return pltpu.roll(x, shift % x.shape[0], 0)


def slot_of(rows):
    return ((131 - lane_of(rows)) // 8) % 16


def two_sum(a, b):
    s = a + b
    t = s - a
    return s, (a - (s - t)) + (b - t)


def quick_sum(a, b):
    s = a + b
    return s, b - (s - a)


def split(a):
    c = a * 4097.0
    high = c - (c - a)
    return high, a - high


def two_prod(a, b):
    p = a * b
    ah, al = split(a)
    bh, bl = split(b)
    return p, ((ah * bh - p) + ah * bl + al * bh) + al * bl


def move_main(main, strip, s):
    lane = lane_of(main.shape[0])
    left = jnp.where(lane == 0, roll_lanes(strip, 8 * s + 1), roll_lanes(main, 1))
    right = jnp.where(lane == LANES - 1, roll_lanes(strip, 8 * s - 1), roll_lanes(main, -1))
    return left, right


def move_strip(mains, strip, second=None):
    rows = strip.shape[0]
    lane = lane_of(rows)
    slot = slot_of(rows)
    edge = jnp.zeros((rows, LANES), F32)
    for s, main in enumerate(mains):
        both = jnp.where(
            lane % 8 == 7, roll_lanes(main, -(8 * s + 1)), roll_lanes(main, 1 - 8 * s)
        )
        edge = jnp.where(slot == s, both, edge)
    left = jnp.where(lane % 8 == 0, edge, roll_lanes(strip, 1))
    right = jnp.where(lane % 8 == 7, edge, roll_lanes(strip, -1))
    if second is not None:
        left = jnp.where(lane % 8 == 4, roll_lanes(second, -3), left)
        right = jnp.where(lane % 8 == 3, roll_lanes(second, 3), right)
    return left, right


def drift(field, left, right, vx, vy):
    along_x = roll_rows(field, -1) - roll_rows(field, 1)
    return -0.5 * (vx * along_x + vy * (right - left))


def strip_speed(vel, count, rows):
    slot = slot_of(rows)
    vx = jnp.zeros((rows, LANES), F32)
    vy = jnp.zeros((rows, LANES), F32)
    for s in range(count):
        vx = jnp.where(slot == s, vel[s, 0], vx)
        vy = jnp.where(slot == s, vel[s, 1], vy)
    return vx, vy


def spread(strip, t):
    lane = lane_of(strip.shape[0])
    source = (LANES - 4 - 8 * t + (lane + 4) % 8) % LANES
    return jnp.take_along_axis(strip, source, axis=1)


def strip_product(get, strip, count):
    total = get(0) * spread(strip, 0)
    for t in range(1, count):
        total = total + get(t) * spread(strip, t)
    return total


def row_product(block, halo, mains, s):
    count = len(mains)
    rows = block.shape[2]
    total = block[s, 0] * mains[0][:rows]
    for t in range(1, count):
        total = total + block[s, t] * mains[t][:rows]
    if halo is None:
        return total
    extra = halo[s * count] * mains[0][rows:]
    for t in range(1, count):
        extra = extra + halo[s * count + t] * mains[t][rows:]
    return jnp.concatenate([total, extra], axis=0)


def first_vector(fields, rates, halo_rates, strips, vel, speed, store):
    state, quad, hist = fields
    count = len(state)
    state_s, quad_s, hist_s, second = strips(2 * count), strips(2 * count + 1), strips(
        2 * count + 2
    ), strips(2 * count + 3)
    for s in range(count):
        left, right = move_main(state[s], state_s, s)
        forcing = drift(state[s], left, right, vel[s, 0], vel[s, 1])
        forcing = forcing + row_product(rates, halo_rates, state, s)
        forcing = forcing - quad[s] * state[s] * state[s]
        store(s, -(state[s] - hist[s] - step_gamma * forcing))
    left, right = move_strip(state, state_s, second)
    forcing = drift(state_s, left, right, *speed)
    forcing = forcing + strip_product(strips, state_s, count)
    forcing = forcing - quad_s * state_s * state_s
    store(None, -(state_s - hist_s - step_gamma * forcing))


def apply_shifted(v, v_s, z, z_s, damp, damp_s, rates, halo_rates, strips, vel, speed, store):
    count = len(z)
    for s in range(count):
        left, right = move_main(z[s], z_s[...], s)
        jac = drift(z[s], left, right, vel[s, 0], vel[s, 1])
        jac = jac + row_product(rates, halo_rates, z, s) - damp(s) * z[s]
        store(s, (z[s] - step_gamma * jac) - v[s])
    z_s = z_s[...]
    left, right = move_strip(z, z_s)
    jac = drift(z_s, left, right, *speed)
    jac = jac + strip_product(strips, z_s, count) - damp_s * z_s
    store(None, (z_s - step_gamma * jac) - v_s)


def pack_kernel(state, history, rates, quadratic, precond, to_right, to_left):
    count, rows, _ = state.shape
    slot = slot_of(rows)
    low = lane_of(rows) % 8 < 4

    def group(index):
        packed = jnp.zeros((rows, LANES), F32)
        for s in range(count):
            if index < count:
                plane = rates[s, index]
            elif index < 2 * count:
                plane = precond[s, index - count]
            else:
                plane = (state, quadratic, history, state)[index - 2 * count][s]
            if index == 2 * count + 3:
                moved = jnp.where(
                    low, roll_lanes(plane, -4 - 8 * s), roll_lanes(plane, 4 - 8 * s)
                )
            else:
                moved = roll_lanes(plane, -8 * s)
            packed = jnp.where(slot == s, moved, packed)
        return packed

    for pair in range(count + 2):
        one, two = group(2 * pair), group(2 * pair + 1)
        to_right[pair] = jnp.where(low, roll_lanes(two, -4), one)
        to_left[pair] = jnp.where(low, one, roll_lanes(two, 4))


def half_kernel(
    from_left, from_right, state, history, rates, quadratic, precond, vel,
    strips_out, send_a, send_b, v_ref, z_ref, vs_ref, zs_ref, *, counts,
):
    count, rows, _ = state.shape
    cols, flip = counts
    low = lane_of(rows) % 8 < 4
    position = lax.axis_index("col")
    has_left = (position > 0).astype(F32)
    has_right = (position < cols - 1).astype(F32)
    for pair in range(count + 2):
        left = from_left[pair] * has_left
        right = from_right[pair] * has_right
        strips_out[2 * pair] = jnp.where(low, right, left)
        strips_out[2 * pair + 1] = jnp.where(low, roll_lanes(right, -4), roll_lanes(left, 4))

    speed = strip_speed(vel, count, rows)
    strips = lambda g: strips_out[g]
    fields = [[ref[s] for s in range(count)] for ref in (state, quadratic, history)]

    def put(k):
        def store(s, value):
            if s is None:
                vs_ref[k] = value
            else:
                v_ref[k, s] = value
        return store

    def precondition(k):
        v = [v_ref[k, s] for s in range(count)]
        for s in range(count):
            z_ref[k, s] = row_product(precond, None, v, s)
        zs_ref[k] = strip_product(lambda t: strips_out[count + t], vs_ref[k], count)

    first_vector(fields, rates, None, strips, vel, speed, put(0))
    precondition(0)
    apply_shifted(
        [v_ref[0, s] for s in range(count)], vs_ref[0],
        [z_ref[0, s] for s in range(count)], zs_ref.at[0],
        lambda s: 2.0 * quadratic[s] * state[s],
        2.0 * strips_out[2 * count + 1] * strips_out[2 * count],
        rates, None, strips, vel, speed, put(1),
    )
    precondition(1)

    odd = (lax.axis_index("parts") % 2) if flip else 0
    for target, near, far in (
        (send_a, (rows - 2) * (1 - odd), (rows - 3) * (1 - odd) + 2 * odd),
        (send_b, (rows - 2) * odd, (rows - 3) * odd + 2 * (1 - odd)),
    ):
        base = 0
        for matrix in (rates, precond):
            for s in range(count):
                for t in range(count):
                    target[base] = matrix[s, t, pl.ds(near, 2), :]
                    base += 1
        for ref in (state, quadratic, history):
            for s in range(count):
                target[base] = ref[s, pl.ds(near, 2), :]
                base += 1
        for g in range(2 * count + 4):
            target[base] = strips_out[g, pl.ds(near, 2), :]
            base += 1
        single = [state.at[s] for s in range(count)]
        single += [z_ref.at[k, s] for k in range(2) for s in range(count)]
        single += [strips_out.at[2 * count], zs_ref.at[0], zs_ref.at[1]]
        for j, ref in enumerate(single):
            target[base + j // 2, pl.ds(j % 2, 1), :] = ref[pl.ds(far, 1), :]
        if len(single) % 2:
            target[base + len(single) // 2, pl.ds(1, 1), :] = jnp.zeros((1, LANES), F32)


def message_planes(count):
    return 2 * count * count + 3 * count + (2 * count + 4) + (3 * count + 3 + 1) // 2


def pairs_of(width):
    return [(i, j) for i in range(width) for j in range(i, width)]


def full_kernel(
    got_a, got_b, strips_in, state, history, rates, quadratic, precond, vel,
    z_out, gram_out,
    halo_rates, halo_precond, fields_ref, strips_ref, inject_ref, inject_s, v_ref, vs_ref,
    zx_ref, zs_ref, *, row_count, flip,
):
    count, rows, _ = state.shape
    ext = rows + 8
    odd = (lax.axis_index("parts") % 2) if flip else 0
    position = lax.axis_index("row")
    above = (position > 0).astype(F32)
    below = (position < row_count - 1).astype(F32)
    odd_f = jnp.asarray(odd).astype(F32)
    keep_a = above * (1 - odd_f) + below * odd_f
    keep_b = below * (1 - odd_f) + above * odd_f
    near_a, far_a = 6 * (1 - odd), 5 * (1 - odd) + 2 * odd
    near_b, far_b = 6 * odd, 5 * odd + 2 * (1 - odd)
    sources = ((got_a, keep_a, near_a, far_a), (got_b, keep_b, near_b, far_b))
    blank = jnp.zeros((8, LANES), F32)

    def receive(target, base, at=0):
        target[pl.ds(at, 8), :] = blank
        for source, keep, near, _ in sources:
            target[pl.ds(at + near, 2), :] = source[base] * keep

    base = 0
    for halo in (halo_rates, halo_precond):
        for k in range(count * count):
            receive(halo.at[k], base)
            base += 1
    for f, ref in enumerate((state, quadratic, history)):
        for s in range(count):
            fields_ref[f, s, 0:rows, :] = ref[s]
            receive(fields_ref.at[f, s], base, rows)
            base += 1
    for g in range(2 * count + 4):
        strips_ref[g, 0:rows, :] = strips_in[g]
        receive(strips_ref.at[g], base, rows)
        base += 1
    single = [(fields_ref.at[0, s], rows) for s in range(count)]
    for k in range(2):
        for s in range(count):
            inject_ref[k, s] = blank
            single.append((inject_ref.at[k, s], 0))
    single.append((strips_ref.at[2 * count], rows))
    for k in range(2):
        inject_s[k] = blank
        single.append((inject_s.at[k], 0))
    for j, (target, at) in enumerate(single):
        for source, keep, _, far in sources:
            target[pl.ds(at + far, 1), :] = source[base + j // 2, pl.ds(j % 2, 1), :] * keep

    speed = strip_speed(vel, count, ext)
    strips = lambda g: strips_ref[g]

    def put(k):
        def store(s, value):
            if s is None:
                vs_ref[k] = value
            else:
                v_ref[k, s] = value
        return store

    fields = [[fields_ref[f, s] for s in range(count)] for f in range(3)]
    first_vector(fields, rates, halo_rates, strips, vel, speed, put(0))

    far_row = (row_of(8) == 2) | (row_of(8) == 5)

    def patch(value, inject):
        return jnp.concatenate(
            [value[:rows], jnp.where(far_row, inject, value[rows:])], axis=0
        )

    for k in range(KRYLOV):
        pick = min(k, 1)
        v = [v_ref[k, s] for s in range(count)]
        for s in range(count):
            value = patch(row_product(precond, halo_precond, v, s), inject_ref[pick, s])
            zx_ref[s] = value
            z_out[k, s] = value[:rows]
        v_s = vs_ref[k]
        z_s = strip_product(lambda t: strips_ref[count + t], v_s, count)
        zs_ref[...] = patch(z_s, inject_s[pick])
        z = [zx_ref[s] for s in range(count)]
        apply_shifted(
            v, v_s, z, zs_ref,
            lambda s: 2.0 * fields_ref[1, s] * fields_ref[0, s],
            2.0 * strips_ref[2 * count + 1] * strips_ref[2 * count],
            rates, halo_rates, strips, vel, speed, put(k + 1),
        )

    pairs = pairs_of(KRYLOV + 1)

    def gather(s, carry):
        high, low = list(carry[0]), list(carry[1])
        for r in range(0, rows, 8):
            whole = [v_ref[k, s, r : r + 8, :] for k in range(KRYLOV + 1)]
            parts = [split(x) for x in whole]
            for n, (i, j) in enumerate(pairs):
                product = parts[i][0] * parts[j][0]
                rest = parts[i][0] * parts[j][1] + parts[i][1] * whole[j]
                high[n], error = two_sum(high[n], product)
                low[n] = low[n] + (error + rest)
        return tuple(high), tuple(low)

    zeros = tuple(blank for _ in pairs)
    high, low = lax.fori_loop(0, count, gather, (zeros, zeros))

    def fold(h, l, shift, move):
        h, error = two_sum(h, move(h, shift))
        return h, l + move(l, shift) + error

    row16, lane16 = row_of(16), lane_of(16)
    top = jnp.zeros((16, LANES), F32)
    bottom = jnp.zeros((16, LANES), F32)
    for n in range(len(pairs)):
        h, l = high[n], low[n]
        for shift in (4, 2, 1):
            h, l = fold(h, l, shift, roll_rows)
        top = jnp.where(row16 == n, jnp.concatenate([h, h], axis=0), top)
        bottom = jnp.where(row16 == n, jnp.concatenate([l, l], axis=0), bottom)
    for shift in (64, 32, 16, 8, 4, 2, 1):
        top, bottom = fold(top, bottom, shift, roll_lanes)
    top, bottom = quick_sum(top, bottom)
    bottom = roll_lanes(bottom, 16)
    line = jnp.where(row16 == lane16, top, 0.0) + jnp.where(row16 + 16 == lane16, bottom, 0.0)
    line = line[:8] + line[8:]
    for shift in (4, 2, 1):
        line = line + roll_rows(line, shift)
    for r in range(0, gram_out.shape[0], 8):
        gram_out[r : r + 8, :] = line


def small_problem(gram):
    width = KRYLOV + 1
    work = dict(gram)
    unit = {}
    pivot = []
    for k in range(width):
        dh, dl = work[k, k]
        pivot.append(jnp.maximum(dh, 0.0))
        inverse = jnp.where(dh > 0.0, 1.0 / jnp.where(dh > 0.0, dh, 1.0), 0.0)
        factor = {}
        for i in range(k + 1, width):
            sh, sl = work[k, i]
            q = sh * inverse
            p, e = two_prod(q, dh)
            rest = ((sh - p) - e) + (sl - q * dl)
            factor[i] = quick_sum(q, rest * inverse)
            unit[k, i] = factor[i][0]
        for i in range(k + 1, width):
            for j in range(i, width):
                fh, fl = factor[i]
                sh, sl = work[k, j]
                p, e = two_prod(fh, sh)
                e = e + (fh * sl + fl * sh)
                wh, wl = work[i, j]
                h, error = two_sum(wh, -p)
                work[i, j] = quick_sum(h, error + (wl - e))
    norm = [jnp.sqrt(d) for d in pivot]
    back = [jnp.where(n > 0.0, 1.0 / jnp.where(n > 0.0, n, 1.0), 0.0) for n in norm]
    inv = {}
    for j in range(KRYLOV):
        column = {j: None}
        inv[j, j] = back[j]
        for i in reversed(range(j)):
            total = unit[i, j] * back[j]
            for m in range(i + 1, j):
                total = total + unit[i, m] * inv[m, j]
            inv[i, j] = -total
    arnoldi = {}
    for j in range(KRYLOV):
        shifted = [inv[0, j]]
        for i in range(1, j + 1):
            shifted.append(inv[i, j] + inv[i - 1, j])
        shifted.append(inv[j, j])
        for i in range(j + 2):
            total = shifted[i]
            for m in range(i + 1, j + 2):
                total = total + unit[i, m] * shifted[m]
            arnoldi[i, j] = norm[i] * total
    beta = jnp.sqrt(pivot[0] + tiny_eps)
    basis = [[norm[0] / beta]]
    hessen = {}
    for k in range(KRYLOV):
        vector = []
        for i in range(k + 2):
            terms = [arnoldi[i, j] * basis[k][j] for j in range(max(i - 1, 0), k + 1)]
            vector.append(functools.reduce(jnp.add, terms))
        for i in range(k + 1):
            terms = [a * b for a, b in zip(basis[i], vector)]
            hessen[i, k] = functools.reduce(jnp.add, terms)
        for m in range(k + 1):
            terms = [hessen[i, k] * basis[i][m] for i in range(m, k + 1)]
            vector[m] = vector[m] - functools.reduce(jnp.add, terms)
        squared = functools.reduce(jnp.add, [x * x for x in vector])
        size = jnp.sqrt(squared + tiny_eps)
        hessen[k + 1, k] = size
        basis.append([x / size for x in vector])
    rotated = [beta] + [jnp.zeros_like(beta)] * KRYLOV
    for k in range(KRYLOV):
        first, second = hessen[k, k], hessen[k + 1, k]
        radius = jnp.sqrt(first * first + second * second)
        cosine, sine = first / radius, second / radius
        for j in range(k, KRYLOV):
            upper = hessen[k, j]
            under = hessen.get((k + 1, j))
            hessen[k, j] = cosine * upper + sine * under
            hessen[k + 1, j] = cosine * under - sine * upper
        rotated[k], rotated[k + 1] = (
            cosine * rotated[k] + sine * rotated[k + 1],
            cosine * rotated[k + 1] - sine * rotated[k],
        )
    coef = [None] * KRYLOV
    for k in reversed(range(KRYLOV)):
        total = rotated[k]
        for j in range(k + 1, KRYLOV):
            total = total - hessen[k, j] * coef[j]
        coef[k] = total / hessen[k, k]
    in_q = [
        functools.reduce(jnp.add, [coef[k] * basis[k][m] for k in range(m, KRYLOV)])
        for m in range(KRYLOV)
    ]
    in_v = [
        functools.reduce(jnp.add, [inv[i, j] * in_q[j] for j in range(i, KRYLOV)])
        for i in range(KRYLOV)
    ]
    return in_v, jnp.abs(rotated[KRYLOV])


def solve_kernel(gathered, z_ref, state, updated, residual):
    count, rows, _ = state.shape
    high = gathered[0:8, :]
    low = roll_lanes(high, -16)
    for r in range(8, gathered.shape[0], 8):
        tile = gathered[r : r + 8, :]
        high, error = two_sum(high, tile)
        low = low + roll_lanes(tile, -16) + error
    for shift in (4, 2, 1):
        high, error = two_sum(high, roll_rows(high, shift))
        low = low + roll_rows(low, shift) + error
    high, low = quick_sum(high, low)
    gram = {}
    for n, pair in enumerate(pairs_of(KRYLOV + 1)):
        gram[pair] = (
            jnp.broadcast_to(high[:, n : n + 1], (8, LANES)),
            jnp.broadcast_to(low[:, n : n + 1], (8, LANES)),
        )
    weights, last = small_problem(gram)
    for s in range(count):
        for r in range(0, rows, 8):
            total = weights[0] * z_ref[0, s, r : r + 8, :]
            for k in range(1, KRYLOV):
                total = total + weights[k] * z_ref[k, s, r : r + 8, :]
            updated[s, r : r + 8, :] = state[s, r : r + 8, :] + total
    residual[:, :] = last


def shapes(*dims):
    return jax.ShapeDtypeStruct(dims, F32)


def body(state, history, rates, quadratic, velocity, precond):
    count, rows, _ = state.shape
    part_count = lax.axis_size("parts")
    row_count = lax.axis_size("row")
    col_count = lax.axis_size("col")
    flip = part_count % 2 == 0
    block = (count, rows, LANES)

    to_right, to_left = pl.pallas_call(
        pack_kernel,
        out_shape=[shapes(count + 2, rows, LANES)] * 2,
        compiler_params=VMEM,
        name="pack_columns",
    )(state, history, rates, quadratic, precond)
    ring = [(i, (i + 1) % col_count) for i in range(col_count)]
    from_left = lax.ppermute(to_right, "col", ring)
    from_right = lax.ppermute(to_left, "col", [(b, a) for a, b in ring])

    smem = pl.BlockSpec(memory_space=pltpu.SMEM)
    whole = pl.BlockSpec(memory_space=pltpu.VMEM)
    planes = message_planes(count)
    strips, send_a, send_b = pl.pallas_call(
        functools.partial(half_kernel, counts=(col_count, flip)),
        in_specs=[whole] * 7 + [smem],
        out_shape=[shapes(2 * count + 4, rows, LANES)] + [shapes(planes, 2, LANES)] * 2,
        scratch_shapes=[
            pltpu.VMEM((2,) + block, F32),
            pltpu.VMEM((2,) + block, F32),
            pltpu.VMEM((2, rows, LANES), F32),
            pltpu.VMEM((2, rows, LANES), F32),
        ],
        compiler_params=VMEM,
        name="half_step",
    )(from_left, from_right, state, history, rates, quadratic, precond, velocity)

    chain = []
    for p in range(part_count):
        for r in range(row_count):
            if flip and p % 2:
                target = (p, r - 1) if r else (p - 1, 0)
            elif flip:
                target = (p, r + 1) if r < row_count - 1 else (p + 1, r)
            else:
                target = (p, (r + 1) % row_count)
            chain.append((p * row_count + r, target[0] * row_count + target[1]))
    got_a = lax.ppermute(send_a, ("parts", "row"), chain)
    got_b = lax.ppermute(send_b, ("parts", "row"), [(b, a) for a, b in chain])

    ext = rows + 8
    members = row_count * col_count
    z, gram = pl.pallas_call(
        functools.partial(full_kernel, row_count=row_count, flip=flip),
        in_specs=[whole] * 8 + [smem],
        out_shape=[shapes(KRYLOV, *block), shapes(members, LANES)],
        scratch_shapes=[
            pltpu.VMEM((count * count, 8, LANES), F32),
            pltpu.VMEM((count * count, 8, LANES), F32),
            pltpu.VMEM((3, count, ext, LANES), F32),
            pltpu.VMEM((2 * count + 4, ext, LANES), F32),
            pltpu.VMEM((2, count, 8, LANES), F32),
            pltpu.VMEM((2, 8, LANES), F32),
            pltpu.VMEM((KRYLOV + 1, count, ext, LANES), F32),
            pltpu.VMEM((KRYLOV + 1, ext, LANES), F32),
            pltpu.VMEM((count, ext, LANES), F32),
            pltpu.VMEM((ext, LANES), F32),
        ],
        compiler_params=VMEM,
        name="krylov",
    )(got_a, got_b, strips, state, history, rates, quadratic, precond, velocity)

    gathered = lax.all_to_all(gram, ("row", "col"), 0, 0, tiled=True)
    updated, last = pl.pallas_call(
        solve_kernel,
        out_shape=[shapes(*block), shapes(8, LANES)],
        compiler_params=VMEM,
        name="solve",
    )(gathered, z, state)
    return updated, last[0, :1]


def solution(mesh):
    placed = (
        P(None, ("parts", "row"), "col"),
        P(None, ("parts", "row"), "col"),
        P(None, None, ("parts", "row"), "col"),
        P(None, ("parts", "row"), "col"),
        P(),
        P(None, None, ("parts", "row"), "col"),
    )
    return jax.shard_map(
        body,
        mesh=mesh,
        in_specs=placed,
        out_specs=(P(None, ("parts", "row"), "col"), P("parts")),
        check_vma=False,
    )
```

```python
import functools

import jax
import jax.numpy as jnp
from jax import lax
from jax.experimental import pallas as pl
from jax.experimental.pallas import tpu as pltpu
from jax.sharding import PartitionSpec as P

KRYLOV = 4
step_gamma = 0.4
tiny_eps = 1e-12

F32 = jnp.float32
LANES = 128
VMEM = pltpu.CompilerParams(vmem_limit_bytes=48 * 1024 * 1024)


def lane_of(rows):
    return lax.broadcasted_iota(jnp.int32, (rows, LANES), 1)


def row_of(rows):
    return lax.broadcasted_iota(jnp.int32, (rows, LANES), 0)


def roll_lanes(x, shift):
    shift %= LANES
    return pltpu.roll(x, shift, 1) if shift else x


def roll_rows(x, shift):
    return pltpu.roll(x, shift % x.shape[0], 0)


def slot_of(rows):
    return ((131 - lane_of(rows)) // 8) % 16


def two_sum(a, b):
    s = a + b
    t = s - a
    return s, (a - (s - t)) + (b - t)


def quick_sum(a, b):
    s = a + b
    return s, b - (s - a)


def split(a):
    c = a * 4097.0
    high = c - (c - a)
    return high, a - high


def two_prod(a, b):
    p = a * b
    ah, al = split(a)
    bh, bl = split(b)
    return p, ((ah * bh - p) + ah * bl + al * bh) + al * bl


def move_main(main, strip, s):
    lane = lane_of(main.shape[0])
    left = jnp.where(lane == 0, roll_lanes(strip, 8 * s + 1), roll_lanes(main, 1))
    right = jnp.where(lane == LANES - 1, roll_lanes(strip, 8 * s - 1), roll_lanes(main, -1))
    return left, right


def move_strip(mains, strip, second=None):
    rows = strip.shape[0]
    lane = lane_of(rows)
    slot = slot_of(rows)
    edge = jnp.zeros((rows, LANES), F32)
    for s, main in enumerate(mains):
        both = jnp.where(
            lane % 8 == 7, roll_lanes(main, -(8 * s + 1)), roll_lanes(main, 1 - 8 * s)
        )
        edge = jnp.where(slot == s, both, edge)
    left = jnp.where(lane % 8 == 0, edge, roll_lanes(strip, 1))
    right = jnp.where(lane % 8 == 7, edge, roll_lanes(strip, -1))
    if second is not None:
        left = jnp.where(lane % 8 == 4, roll_lanes(second, -3), left)
        right = jnp.where(lane % 8 == 3, roll_lanes(second, 3), right)
    return left, right


def drift(field, left, right, vx, vy):
    along_x = roll_rows(field, -1) - roll_rows(field, 1)
    return -0.5 * (vx * along_x + vy * (right - left))


def strip_speed(vel, count, rows):
    slot = slot_of(rows)
    vx = jnp.zeros((rows, LANES), F32)
    vy = jnp.zeros((rows, LANES), F32)
    for s in range(count):
        vx = jnp.where(slot == s, vel[s, 0], vx)
        vy = jnp.where(slot == s, vel[s, 1], vy)
    return vx, vy


def spread(strip, t):
    lane = lane_of(strip.shape[0])
    source = (LANES - 4 - 8 * t + (lane + 4) % 8) % LANES
    return jnp.take_along_axis(strip, source, axis=1)


def strip_product(get, strip, count):
    total = get(0) * spread(strip, 0)
    for t in range(1, count):
        total = total + get(t) * spread(strip, t)
    return total


def row_product(block, halo, mains, s):
    count = len(mains)
    rows = block.shape[2]
    total = block[s, 0] * mains[0][:rows]
    for t in range(1, count):
        total = total + block[s, t] * mains[t][:rows]
    if halo is None:
        return total
    extra = halo[s * count] * mains[0][rows:]
    for t in range(1, count):
        extra = extra + halo[s * count + t] * mains[t][rows:]
    return jnp.concatenate([total, extra], axis=0)


def first_vector(fields, rates, halo_rates, strips, vel, speed, store):
    state, quad, hist = fields
    count = len(state)
    state_s, quad_s, hist_s, second = strips(2 * count), strips(2 * count + 1), strips(
        2 * count + 2
    ), strips(2 * count + 3)
    for s in range(count):
        left, right = move_main(state[s], state_s, s)
        forcing = drift(state[s], left, right, vel[s, 0], vel[s, 1])
        forcing = forcing + row_product(rates, halo_rates, state, s)
        forcing = forcing - quad[s] * state[s] * state[s]
        store(s, -(state[s] - hist[s] - step_gamma * forcing))
    left, right = move_strip(state, state_s, second)
    forcing = drift(state_s, left, right, *speed)
    forcing = forcing + strip_product(strips, state_s, count)
    forcing = forcing - quad_s * state_s * state_s
    store(None, -(state_s - hist_s - step_gamma * forcing))


def apply_shifted(v, v_s, z, z_s, damp, damp_s, rates, halo_rates, strips, vel, speed, store):
    count = len(z)
    for s in range(count):
        left, right = move_main(z[s], z_s[...], s)
        jac = drift(z[s], left, right, vel[s, 0], vel[s, 1])
        jac = jac + row_product(rates, halo_rates, z, s) - damp(s) * z[s]
        store(s, (z[s] - step_gamma * jac) - v[s])
    z_s = z_s[...]
    left, right = move_strip(z, z_s)
    jac = drift(z_s, left, right, *speed)
    jac = jac + strip_product(strips, z_s, count) - damp_s * z_s
    store(None, (z_s - step_gamma * jac) - v_s)


def pack_kernel(
    state_in, history_in, rates_in, quadratic_in, precond_in,
    state, history, rates, quadratic, precond, to_right, to_left, sems,
):
    count, rows, _ = state.shape
    copies = [
        pltpu.make_async_copy(source, target, sems.at[n])
        for n, (source, target) in enumerate(
            (
                (rates_in, rates),
                (precond_in, precond),
                (state_in, state),
                (quadratic_in, quadratic),
                (history_in, history),
            )
        )
    ]
    for copy in copies:
        copy.start()
    slot = slot_of(rows)
    low = lane_of(rows) % 8 < 4

    def group(index):
        packed = jnp.zeros((rows, LANES), F32)
        for s in range(count):
            if index < count:
                plane = rates[s, index]
            elif index < 2 * count:
                plane = precond[s, index - count]
            else:
                plane = (state, quadratic, history, state)[index - 2 * count][s]
            if index == 2 * count + 3:
                moved = jnp.where(
                    low, roll_lanes(plane, -4 - 8 * s), roll_lanes(plane, 4 - 8 * s)
                )
            else:
                moved = roll_lanes(plane, -8 * s)
            packed = jnp.where(slot == s, moved, packed)
        return packed

    done = set()
    for pair in range(count + 2):
        ready = 1 if 2 * pair + 1 < count else 2 if 2 * pair + 1 < 2 * count else 5
        for n in range(ready):
            if n not in done:
                copies[n].wait()
                done.add(n)
        one, two = group(2 * pair), group(2 * pair + 1)
        to_right[pair] = jnp.where(low, roll_lanes(two, -4), one)
        to_left[pair] = jnp.where(low, one, roll_lanes(two, 4))


def half_kernel(
    from_left, from_right, state, history, rates, quadratic, precond, vel,
    strips_out, send_a, send_b, v_ref, z_ref, vs_ref, zs_ref, *, counts,
):
    count, rows, _ = state.shape
    cols, flip = counts
    low = lane_of(rows) % 8 < 4
    position = lax.axis_index("col")
    has_left = (position > 0).astype(F32)
    has_right = (position < cols - 1).astype(F32)
    for pair in range(count + 2):
        left = from_left[pair] * has_left
        right = from_right[pair] * has_right
        strips_out[2 * pair] = jnp.where(low, right, left)
        strips_out[2 * pair + 1] = jnp.where(low, roll_lanes(right, -4), roll_lanes(left, 4))

    speed = strip_speed(vel, count, rows)
    strips = lambda g: strips_out[g]
    fields = [[ref[s] for s in range(count)] for ref in (state, quadratic, history)]

    def put(k):
        def store(s, value):
            if s is None:
                vs_ref[k] = value
            else:
                v_ref[k, s] = value
        return store

    def precondition(k):
        v = [v_ref[k, s] for s in range(count)]
        for s in range(count):
            z_ref[k, s] = row_product(precond, None, v, s)
        zs_ref[k] = strip_product(lambda t: strips_out[count + t], vs_ref[k], count)

    first_vector(fields, rates, None, strips, vel, speed, put(0))
    precondition(0)
    apply_shifted(
        [v_ref[0, s] for s in range(count)], vs_ref[0],
        [z_ref[0, s] for s in range(count)], zs_ref.at[0],
        lambda s: 2.0 * quadratic[s] * state[s],
        2.0 * strips_out[2 * count + 1] * strips_out[2 * count],
        rates, None, strips, vel, speed, put(1),
    )
    precondition(1)

    odd = (lax.axis_index("parts") % 2) if flip else 0
    for target, near, far in (
        (send_a, (rows - 2) * (1 - odd), (rows - 3) * (1 - odd) + 2 * odd),
        (send_b, (rows - 2) * odd, (rows - 3) * odd + 2 * (1 - odd)),
    ):
        base = 0
        for matrix in (rates, precond):
            for s in range(count):
                for t in range(count):
                    target[base] = matrix[s, t, pl.ds(near, 2), :]
                    base += 1
        for ref in (state, quadratic, history):
            for s in range(count):
                target[base] = ref[s, pl.ds(near, 2), :]
                base += 1
        for g in range(2 * count + 4):
            target[base] = strips_out[g, pl.ds(near, 2), :]
            base += 1
        single = [state.at[s] for s in range(count)]
        single += [z_ref.at[k, s] for k in range(2) for s in range(count)]
        single += [strips_out.at[2 * count], zs_ref.at[0], zs_ref.at[1]]
        for j, ref in enumerate(single):
            target[base + j // 2, pl.ds(j % 2, 1), :] = ref[pl.ds(far, 1), :]
        if len(single) % 2:
            target[base + len(single) // 2, pl.ds(1, 1), :] = jnp.zeros((1, LANES), F32)


def message_planes(count):
    return 2 * count * count + 3 * count + (2 * count + 4) + (3 * count + 3 + 1) // 2


def pairs_of(width):
    return [(i, j) for i in range(width) for j in range(i, width)]


def full_kernel(
    got_a, got_b, strips_in, state, history, rates, quadratic, precond, vel,
    z_out, gram_out,
    halo_rates, halo_precond, fields_ref, strips_ref, inject_ref, inject_s, v_ref, vs_ref,
    zx_ref, zs_ref, *, row_count, flip,
):
    count, rows, _ = state.shape
    ext = rows + 8
    odd = (lax.axis_index("parts") % 2) if flip else 0
    position = lax.axis_index("row")
    above = (position > 0).astype(F32)
    below = (position < row_count - 1).astype(F32)
    odd_f = jnp.asarray(odd).astype(F32)
    keep_a = above * (1 - odd_f) + below * odd_f
    keep_b = below * (1 - odd_f) + above * odd_f
    near_a, far_a = 6 * (1 - odd), 5 * (1 - odd) + 2 * odd
    near_b, far_b = 6 * odd, 5 * odd + 2 * (1 - odd)
    sources = ((got_a, keep_a, near_a, far_a), (got_b, keep_b, near_b, far_b))
    blank = jnp.zeros((8, LANES), F32)

    def receive(target, base, at=0):
        target[pl.ds(at, 8), :] = blank
        for source, keep, near, _ in sources:
            target[pl.ds(at + near, 2), :] = source[base] * keep

    base = 0
    for halo in (halo_rates, halo_precond):
        for k in range(count * count):
            receive(halo.at[k], base)
            base += 1
    for f, ref in enumerate((state, quadratic, history)):
        for s in range(count):
            fields_ref[f, s, 0:rows, :] = ref[s]
            receive(fields_ref.at[f, s], base, rows)
            base += 1
    for g in range(2 * count + 4):
        strips_ref[g, 0:rows, :] = strips_in[g]
        receive(strips_ref.at[g], base, rows)
        base += 1
    single = [(fields_ref.at[0, s], rows) for s in range(count)]
    for k in range(2):
        for s in range(count):
            inject_ref[k, s] = blank
            single.append((inject_ref.at[k, s], 0))
    single.append((strips_ref.at[2 * count], rows))
    for k in range(2):
        inject_s[k] = blank
        single.append((inject_s.at[k], 0))
    for j, (target, at) in enumerate(single):
        for source, keep, _, far in sources:
            target[pl.ds(at + far, 1), :] = source[base + j // 2, pl.ds(j % 2, 1), :] * keep

    speed = strip_speed(vel, count, ext)
    strips = lambda g: strips_ref[g]

    def put(k):
        def store(s, value):
            if s is None:
                vs_ref[k] = value
            else:
                v_ref[k, s] = value
        return store

    fields = [[fields_ref[f, s] for s in range(count)] for f in range(3)]
    first_vector(fields, rates, halo_rates, strips, vel, speed, put(0))

    far_row = (row_of(8) == 2) | (row_of(8) == 5)

    def patch(value, inject):
        return jnp.concatenate(
            [value[:rows], jnp.where(far_row, inject, value[rows:])], axis=0
        )

    for k in range(KRYLOV):
        pick = min(k, 1)
        v = [v_ref[k, s] for s in range(count)]
        for s in range(count):
            value = patch(row_product(precond, halo_precond, v, s), inject_ref[pick, s])
            zx_ref[s] = value
            z_out[k, s] = value[:rows]
        v_s = vs_ref[k]
        z_s = strip_product(lambda t: strips_ref[count + t], v_s, count)
        zs_ref[...] = patch(z_s, inject_s[pick])
        z = [zx_ref[s] for s in range(count)]
        apply_shifted(
            v, v_s, z, zs_ref,
            lambda s: 2.0 * fields_ref[1, s] * fields_ref[0, s],
            2.0 * strips_ref[2 * count + 1] * strips_ref[2 * count],
            rates, halo_rates, strips, vel, speed, put(k + 1),
        )

    pairs = pairs_of(KRYLOV + 1)

    def gather(s, carry):
        high, low = list(carry[0]), list(carry[1])
        for r in range(0, rows, 8):
            whole = [v_ref[k, s, r : r + 8, :] for k in range(KRYLOV + 1)]
            parts = [split(x) for x in whole]
            for n, (i, j) in enumerate(pairs):
                product = parts[i][0] * parts[j][0]
                rest = parts[i][0] * parts[j][1] + parts[i][1] * whole[j]
                high[n], error = two_sum(high[n], product)
                low[n] = low[n] + (error + rest)
        return tuple(high), tuple(low)

    zeros = tuple(blank for _ in pairs)
    high, low = lax.fori_loop(0, count, gather, (zeros, zeros))

    def fold(h, l, shift, move):
        h, error = two_sum(h, move(h, shift))
        return h, l + move(l, shift) + error

    row16, lane16 = row_of(16), lane_of(16)
    top = jnp.zeros((16, LANES), F32)
    bottom = jnp.zeros((16, LANES), F32)
    for n in range(len(pairs)):
        h, l = high[n], low[n]
        for shift in (4, 2, 1):
            h, l = fold(h, l, shift, roll_rows)
        top = jnp.where(row16 == n, jnp.concatenate([h, h], axis=0), top)
        bottom = jnp.where(row16 == n, jnp.concatenate([l, l], axis=0), bottom)
    for shift in (64, 32, 16, 8, 4, 2, 1):
        top, bottom = fold(top, bottom, shift, roll_lanes)
    top, bottom = quick_sum(top, bottom)
    bottom = roll_lanes(bottom, 16)
    line = jnp.where(row16 == lane16, top, 0.0) + jnp.where(row16 + 16 == lane16, bottom, 0.0)
    line = line[:8] + line[8:]
    for shift in (4, 2, 1):
        line = line + roll_rows(line, shift)
    for r in range(0, gram_out.shape[0], 8):
        gram_out[r : r + 8, :] = line


def small_problem(gram):
    width = KRYLOV + 1
    work = dict(gram)
    unit = {}
    pivot = []
    for k in range(width):
        dh, dl = work[k, k]
        pivot.append(jnp.maximum(dh, 0.0))
        inverse = jnp.where(dh > 0.0, 1.0 / jnp.where(dh > 0.0, dh, 1.0), 0.0)
        factor = {}
        for i in range(k + 1, width):
            sh, sl = work[k, i]
            q = sh * inverse
            p, e = two_prod(q, dh)
            rest = ((sh - p) - e) + (sl - q * dl)
            factor[i] = quick_sum(q, rest * inverse)
            unit[k, i] = factor[i][0]
        for i in range(k + 1, width):
            for j in range(i, width):
                fh, fl = factor[i]
                sh, sl = work[k, j]
                p, e = two_prod(fh, sh)
                e = e + (fh * sl + fl * sh)
                wh, wl = work[i, j]
                h, error = two_sum(wh, -p)
                work[i, j] = quick_sum(h, error + (wl - e))
    norm = [jnp.sqrt(d) for d in pivot]
    back = [jnp.where(n > 0.0, 1.0 / jnp.where(n > 0.0, n, 1.0), 0.0) for n in norm]
    inv = {}
    for j in range(KRYLOV):
        column = {j: None}
        inv[j, j] = back[j]
        for i in reversed(range(j)):
            total = unit[i, j] * back[j]
            for m in range(i + 1, j):
                total = total + unit[i, m] * inv[m, j]
            inv[i, j] = -total
    arnoldi = {}
    for j in range(KRYLOV):
        shifted = [inv[0, j]]
        for i in range(1, j + 1):
            shifted.append(inv[i, j] + inv[i - 1, j])
        shifted.append(inv[j, j])
        for i in range(j + 2):
            total = shifted[i]
            for m in range(i + 1, j + 2):
                total = total + unit[i, m] * shifted[m]
            arnoldi[i, j] = norm[i] * total
    beta = jnp.sqrt(pivot[0] + tiny_eps)
    basis = [[norm[0] / beta]]
    hessen = {}
    for k in range(KRYLOV):
        vector = []
        for i in range(k + 2):
            terms = [arnoldi[i, j] * basis[k][j] for j in range(max(i - 1, 0), k + 1)]
            vector.append(functools.reduce(jnp.add, terms))
        for i in range(k + 1):
            terms = [a * b for a, b in zip(basis[i], vector)]
            hessen[i, k] = functools.reduce(jnp.add, terms)
        for m in range(k + 1):
            terms = [hessen[i, k] * basis[i][m] for i in range(m, k + 1)]
            vector[m] = vector[m] - functools.reduce(jnp.add, terms)
        squared = functools.reduce(jnp.add, [x * x for x in vector])
        size = jnp.sqrt(squared + tiny_eps)
        hessen[k + 1, k] = size
        basis.append([x / size for x in vector])
    rotated = [beta] + [jnp.zeros_like(beta)] * KRYLOV
    for k in range(KRYLOV):
        first, second = hessen[k, k], hessen[k + 1, k]
        radius = jnp.sqrt(first * first + second * second)
        cosine, sine = first / radius, second / radius
        for j in range(k, KRYLOV):
            upper = hessen[k, j]
            under = hessen.get((k + 1, j))
            hessen[k, j] = cosine * upper + sine * under
            hessen[k + 1, j] = cosine * under - sine * upper
        rotated[k], rotated[k + 1] = (
            cosine * rotated[k] + sine * rotated[k + 1],
            cosine * rotated[k + 1] - sine * rotated[k],
        )
    coef = [None] * KRYLOV
    for k in reversed(range(KRYLOV)):
        total = rotated[k]
        for j in range(k + 1, KRYLOV):
            total = total - hessen[k, j] * coef[j]
        coef[k] = total / hessen[k, k]
    in_q = [
        functools.reduce(jnp.add, [coef[k] * basis[k][m] for k in range(m, KRYLOV)])
        for m in range(KRYLOV)
    ]
    in_v = [
        functools.reduce(jnp.add, [inv[i, j] * in_q[j] for j in range(i, KRYLOV)])
        for i in range(KRYLOV)
    ]
    return in_v, jnp.abs(rotated[KRYLOV])


def solve_kernel(gathered, z_ref, state, updated, residual):
    count, rows, _ = state.shape
    high = gathered[0:8, :]
    low = roll_lanes(high, -16)
    for r in range(8, gathered.shape[0], 8):
        tile = gathered[r : r + 8, :]
        high, error = two_sum(high, tile)
        low = low + roll_lanes(tile, -16) + error
    for shift in (4, 2, 1):
        high, error = two_sum(high, roll_rows(high, shift))
        low = low + roll_rows(low, shift) + error
    high, low = quick_sum(high, low)
    gram = {}
    for n, pair in enumerate(pairs_of(KRYLOV + 1)):
        gram[pair] = (
            jnp.broadcast_to(high[:, n : n + 1], (8, LANES)),
            jnp.broadcast_to(low[:, n : n + 1], (8, LANES)),
        )
    weights, last = small_problem(gram)
    for s in range(count):
        for r in range(0, rows, 8):
            total = weights[0] * z_ref[0, s, r : r + 8, :]
            for k in range(1, KRYLOV):
                total = total + weights[k] * z_ref[k, s, r : r + 8, :]
            updated[s, r : r + 8, :] = state[s, r : r + 8, :] + total
    residual[0] = last[0, 0]


def shapes(*dims):
    return jax.ShapeDtypeStruct(dims, F32)


def body(state, history, rates, quadratic, velocity, precond):
    count, rows, _ = state.shape
    part_count = lax.axis_size("parts")
    row_count = lax.axis_size("row")
    col_count = lax.axis_size("col")
    flip = part_count % 2 == 0
    block = (count, rows, LANES)

    square = (count,) + block
    smem = pl.BlockSpec(memory_space=pltpu.SMEM)
    whole = pl.BlockSpec(memory_space=pltpu.VMEM)
    inputs = [
        pltpu.with_memory_space_constraint(x, pltpu.HBM)
        for x in (state, history, rates, quadratic, precond)
    ]
    state, history, rates, quadratic, precond, to_right, to_left = pl.pallas_call(
        pack_kernel,
        in_specs=[pl.BlockSpec(memory_space=pltpu.HBM)] * 5,
        out_shape=[
            shapes(*block), shapes(*block), shapes(*square), shapes(*block), shapes(*square),
            shapes(count + 2, rows, LANES), shapes(count + 2, rows, LANES),
        ],
        out_specs=[whole] * 7,
        scratch_shapes=[pltpu.SemaphoreType.DMA((5,))],
        compiler_params=VMEM,
        name="pack_columns",
    )(*inputs)
    ring = [(i, (i + 1) % col_count) for i in range(col_count)]
    from_left = lax.ppermute(to_right, "col", ring)
    from_right = lax.ppermute(to_left, "col", [(b, a) for a, b in ring])

    planes = message_planes(count)
    strips, send_a, send_b = pl.pallas_call(
        functools.partial(half_kernel, counts=(col_count, flip)),
        in_specs=[whole] * 7 + [smem],
        out_shape=[shapes(2 * count + 4, rows, LANES)] + [shapes(planes, 2, LANES)] * 2,
        scratch_shapes=[
            pltpu.VMEM((2,) + block, F32),
            pltpu.VMEM((2,) + block, F32),
            pltpu.VMEM((2, rows, LANES), F32),
            pltpu.VMEM((2, rows, LANES), F32),
        ],
        compiler_params=VMEM,
        name="half_step",
    )(from_left, from_right, state, history, rates, quadratic, precond, velocity)

    chain = []
    for p in range(part_count):
        for r in range(row_count):
            if flip and p % 2:
                target = (p, r - 1) if r else (p - 1, 0)
            elif flip:
                target = (p, r + 1) if r < row_count - 1 else (p + 1, r)
            else:
                target = (p, (r + 1) % row_count)
            chain.append((p * row_count + r, target[0] * row_count + target[1]))
    got_a = lax.ppermute(send_a, ("parts", "row"), chain)
    got_b = lax.ppermute(send_b, ("parts", "row"), [(b, a) for a, b in chain])

    ext = rows + 8
    members = row_count * col_count
    z, gram = pl.pallas_call(
        functools.partial(full_kernel, row_count=row_count, flip=flip),
        in_specs=[whole] * 8 + [smem],
        out_shape=[shapes(KRYLOV, *block), shapes(members, LANES)],
        scratch_shapes=[
            pltpu.VMEM((count * count, 8, LANES), F32),
            pltpu.VMEM((count * count, 8, LANES), F32),
            pltpu.VMEM((3, count, ext, LANES), F32),
            pltpu.VMEM((2 * count + 4, ext, LANES), F32),
            pltpu.VMEM((2, count, 8, LANES), F32),
            pltpu.VMEM((2, 8, LANES), F32),
            pltpu.VMEM((KRYLOV + 1, count, ext, LANES), F32),
            pltpu.VMEM((KRYLOV + 1, ext, LANES), F32),
            pltpu.VMEM((count, ext, LANES), F32),
            pltpu.VMEM((ext, LANES), F32),
        ],
        compiler_params=VMEM,
        name="krylov",
    )(got_a, got_b, strips, state, history, rates, quadratic, precond, velocity)

    gathered = lax.all_to_all(gram, ("row", "col"), 0, 0, tiled=True)
    updated, last = pl.pallas_call(
        solve_kernel,
        out_shape=[shapes(*block), shapes(1)],
        out_specs=[whole, smem],
        compiler_params=VMEM,
        name="solve",
    )(gathered, z, state)
    return updated, last


def solution(mesh):
    placed = (
        P(None, ("parts", "row"), "col"),
        P(None, ("parts", "row"), "col"),
        P(None, None, ("parts", "row"), "col"),
        P(None, ("parts", "row"), "col"),
        P(),
        P(None, None, ("parts", "row"), "col"),
    )
    return jax.shard_map(
        body,
        mesh=mesh,
        in_specs=placed,
        out_specs=(P(None, ("parts", "row"), "col"), P("parts")),
        check_vma=False,
    )
```

```python
import functools

import jax
import jax.numpy as jnp
from jax import lax
from jax.experimental import pallas as pl
from jax.experimental.pallas import tpu as pltpu
from jax.sharding import PartitionSpec as P

KRYLOV = 4
step_gamma = 0.4
tiny_eps = 1e-12

F32 = jnp.float32
LANES = 128
VMEM = pltpu.CompilerParams(vmem_limit_bytes=48 * 1024 * 1024)


def lane_of(rows):
    return lax.broadcasted_iota(jnp.int32, (rows, LANES), 1)


def row_of(rows):
    return lax.broadcasted_iota(jnp.int32, (rows, LANES), 0)


def roll_lanes(x, shift):
    shift %= LANES
    return pltpu.roll(x, shift, 1) if shift else x


def roll_rows(x, shift):
    return pltpu.roll(x, shift % x.shape[0], 0)


def slot_of(rows):
    return ((131 - lane_of(rows)) // 8) % 16


def two_sum(a, b):
    s = a + b
    t = s - a
    return s, (a - (s - t)) + (b - t)


def quick_sum(a, b):
    s = a + b
    return s, b - (s - a)


def split(a):
    c = a * 4097.0
    high = c - (c - a)
    return high, a - high


def two_prod(a, b):
    p = a * b
    ah, al = split(a)
    bh, bl = split(b)
    return p, ((ah * bh - p) + ah * bl + al * bh) + al * bl


def move_main(main, strip, s):
    lane = lane_of(main.shape[0])
    left = jnp.where(lane == 0, roll_lanes(strip, 8 * s + 1), roll_lanes(main, 1))
    right = jnp.where(lane == LANES - 1, roll_lanes(strip, 8 * s - 1), roll_lanes(main, -1))
    return left, right


def move_strip(mains, strip, second=None):
    rows = strip.shape[0]
    lane = lane_of(rows)
    slot = slot_of(rows)
    edge = jnp.zeros((rows, LANES), F32)
    for s, main in enumerate(mains):
        both = jnp.where(
            lane % 8 == 7, roll_lanes(main, -(8 * s + 1)), roll_lanes(main, 1 - 8 * s)
        )
        edge = jnp.where(slot == s, both, edge)
    left = jnp.where(lane % 8 == 0, edge, roll_lanes(strip, 1))
    right = jnp.where(lane % 8 == 7, edge, roll_lanes(strip, -1))
    if second is not None:
        left = jnp.where(lane % 8 == 4, roll_lanes(second, -3), left)
        right = jnp.where(lane % 8 == 3, roll_lanes(second, 3), right)
    return left, right


def drift(field, left, right, vx, vy):
    along_x = roll_rows(field, -1) - roll_rows(field, 1)
    return -0.5 * (vx * along_x + vy * (right - left))


def strip_speed(vel, count, rows):
    slot = slot_of(rows)
    vx = jnp.zeros((rows, LANES), F32)
    vy = jnp.zeros((rows, LANES), F32)
    for s in range(count):
        vx = jnp.where(slot == s, vel[s, 0], vx)
        vy = jnp.where(slot == s, vel[s, 1], vy)
    return vx, vy


def spread(strip, t):
    lane = lane_of(strip.shape[0])
    source = (LANES - 4 - 8 * t + (lane + 4) % 8) % LANES
    return jnp.take_along_axis(strip, source, axis=1)


def strip_product(get, strip, count):
    total = get(0) * spread(strip, 0)
    for t in range(1, count):
        total = total + get(t) * spread(strip, t)
    return total


def row_product(block, halo, mains, s):
    count = len(mains)
    rows = block.shape[2]
    total = block[s, 0] * mains[0][:rows]
    for t in range(1, count):
        total = total + block[s, t] * mains[t][:rows]
    if halo is None:
        return total
    extra = halo[s * count] * mains[0][rows:]
    for t in range(1, count):
        extra = extra + halo[s * count + t] * mains[t][rows:]
    return jnp.concatenate([total, extra], axis=0)


def first_vector(fields, rates, halo_rates, strips, vel, speed, store):
    state, quad, hist = fields
    count = len(state)
    state_s, quad_s, hist_s, second = strips(2 * count), strips(2 * count + 1), strips(
        2 * count + 2
    ), strips(2 * count + 3)
    for s in range(count):
        left, right = move_main(state[s], state_s, s)
        forcing = drift(state[s], left, right, vel[s, 0], vel[s, 1])
        forcing = forcing + row_product(rates, halo_rates, state, s)
        forcing = forcing - quad[s] * state[s] * state[s]
        store(s, -(state[s] - hist[s] - step_gamma * forcing))
    left, right = move_strip(state, state_s, second)
    forcing = drift(state_s, left, right, *speed)
    forcing = forcing + strip_product(strips, state_s, count)
    forcing = forcing - quad_s * state_s * state_s
    store(None, -(state_s - hist_s - step_gamma * forcing))


def apply_shifted(v, v_s, z, z_s, damp, damp_s, rates, halo_rates, strips, vel, speed, store):
    count = len(z)
    for s in range(count):
        left, right = move_main(z[s], z_s[...], s)
        jac = drift(z[s], left, right, vel[s, 0], vel[s, 1])
        jac = jac + row_product(rates, halo_rates, z, s) - damp(s) * z[s]
        store(s, (z[s] - step_gamma * jac) - v[s])
    z_s = z_s[...]
    left, right = move_strip(z, z_s)
    jac = drift(z_s, left, right, *speed)
    jac = jac + strip_product(strips, z_s, count) - damp_s * z_s
    store(None, (z_s - step_gamma * jac) - v_s)


def edge_rows(rows, flip):
    odd = (lax.axis_index("parts") % 2) if flip else 0
    down, up = (rows - 2, rows - 3), (0, 2)
    return tuple(
        tuple(x + (y - x) * odd for x, y in zip(*ends)) for ends in ((down, up), (up, down))
    )


def pack_kernel(
    state_in, history_in, rates_in, quadratic_in, precond_in,
    state, history, rates, quadratic, precond, to_right, to_left, raw_a, raw_b, sems, *, flip,
):
    count, rows, _ = state.shape
    copies = [
        pltpu.make_async_copy(source, target, sems.at[n])
        for n, (source, target) in enumerate(
            (
                (rates_in, rates),
                (precond_in, precond),
                (state_in, state),
                (quadratic_in, quadratic),
                (history_in, history),
            )
        )
    ]
    for copy in copies:
        copy.start()
    slot = slot_of(rows)
    low = lane_of(rows) % 8 < 4

    def group(index):
        packed = jnp.zeros((rows, LANES), F32)
        for s in range(count):
            if index < count:
                plane = rates[s, index]
            elif index < 2 * count:
                plane = precond[s, index - count]
            else:
                plane = (state, quadratic, history, state)[index - 2 * count][s]
            if index == 2 * count + 3:
                moved = jnp.where(
                    low, roll_lanes(plane, -4 - 8 * s), roll_lanes(plane, 4 - 8 * s)
                )
            else:
                moved = roll_lanes(plane, -8 * s)
            packed = jnp.where(slot == s, moved, packed)
        return packed

    done = set()
    for pair in range(count + 2):
        ready = 1 if 2 * pair + 1 < count else 2 if 2 * pair + 1 < 2 * count else 5
        for n in range(ready):
            if n not in done:
                copies[n].wait()
                done.add(n)
        one, two = group(2 * pair), group(2 * pair + 1)
        to_right[pair] = jnp.where(low, roll_lanes(two, -4), one)
        to_left[pair] = jnp.where(low, one, roll_lanes(two, 4))

    for target, (near, _) in zip((raw_a, raw_b), edge_rows(rows, flip)):
        planes = [m.at[s, t] for m in (rates, precond) for s in range(count) for t in range(count)]
        planes += [ref.at[s] for ref in (state, quadratic, history) for s in range(count)]
        for n, ref in enumerate(planes):
            target[n] = ref[pl.ds(near, 2), :]


def half_kernel(
    from_left, from_right, state, history, rates, quadratic, precond, vel,
    strips_out, send_a, send_b, v_ref, z_ref, vs_ref, zs_ref, *, counts,
):
    count, rows, _ = state.shape
    cols, flip = counts
    low = lane_of(rows) % 8 < 4
    position = lax.axis_index("col")
    has_left = (position > 0).astype(F32)
    has_right = (position < cols - 1).astype(F32)
    for pair in range(count + 2):
        left = from_left[pair] * has_left
        right = from_right[pair] * has_right
        strips_out[2 * pair] = jnp.where(low, right, left)
        strips_out[2 * pair + 1] = jnp.where(low, roll_lanes(right, -4), roll_lanes(left, 4))

    speed = strip_speed(vel, count, rows)
    strips = lambda g: strips_out[g]
    fields = [[ref[s] for s in range(count)] for ref in (state, quadratic, history)]

    def put(k):
        def store(s, value):
            if s is None:
                vs_ref[k] = value
            else:
                v_ref[k, s] = value
        return store

    def precondition(k):
        v = [v_ref[k, s] for s in range(count)]
        for s in range(count):
            z_ref[k, s] = row_product(precond, None, v, s)
        zs_ref[k] = strip_product(lambda t: strips_out[count + t], vs_ref[k], count)

    first_vector(fields, rates, None, strips, vel, speed, put(0))
    precondition(0)
    apply_shifted(
        [v_ref[0, s] for s in range(count)], vs_ref[0],
        [z_ref[0, s] for s in range(count)], zs_ref.at[0],
        lambda s: 2.0 * quadratic[s] * state[s],
        2.0 * strips_out[2 * count + 1] * strips_out[2 * count],
        rates, None, strips, vel, speed, put(1),
    )
    precondition(1)

    single = [state.at[s] for s in range(count)]
    single += [z_ref.at[k, s] for k in range(2) for s in range(count)]
    single += [strips_out.at[2 * count], zs_ref.at[0], zs_ref.at[1]]
    base = 2 * count + 4
    for target, (near, far) in zip((send_a, send_b), edge_rows(rows, flip)):
        for g in range(base):
            target[g] = strips_out[g, pl.ds(near, 2), :]
        for j, ref in enumerate(single):
            target[base + j // 2, pl.ds(j % 2, 1), :] = ref[pl.ds(far, 1), :]
        if len(single) % 2:
            target[base + len(single) // 2, pl.ds(1, 1), :] = jnp.zeros((1, LANES), F32)


def raw_planes(count):
    return 2 * count * count + 3 * count


def message_planes(count):
    return (2 * count + 4) + (3 * count + 3 + 1) // 2


def pairs_of(width):
    return [(i, j) for i in range(width) for j in range(i, width)]


def full_kernel(
    raw_a, raw_b, got_a, got_b, strips_in, state, history, rates, quadratic, precond, vel,
    z_out, gram_out,
    halo_rates, halo_precond, fields_ref, strips_ref, inject_ref, inject_s, v_ref, vs_ref,
    zx_ref, zs_ref, *, row_count, flip,
):
    count, rows, _ = state.shape
    ext = rows + 8
    odd = (lax.axis_index("parts") % 2) if flip else 0
    position = lax.axis_index("row")
    above = (position > 0).astype(F32)
    below = (position < row_count - 1).astype(F32)
    odd_f = jnp.asarray(odd).astype(F32)
    keep_a = above * (1 - odd_f) + below * odd_f
    keep_b = below * (1 - odd_f) + above * odd_f
    near_a, far_a = 6 * (1 - odd), 5 * (1 - odd) + 2 * odd
    near_b, far_b = 6 * odd, 5 * odd + 2 * (1 - odd)
    raws = ((raw_a, keep_a, near_a), (raw_b, keep_b, near_b))
    sources = ((got_a, keep_a, near_a, far_a), (got_b, keep_b, near_b, far_b))
    blank = jnp.zeros((8, LANES), F32)

    def receive(target, base, at=0, sources=raws):
        target[pl.ds(at, 8), :] = blank
        for source, keep, near, *_ in sources:
            target[pl.ds(at + near, 2), :] = source[base] * keep

    base = 0
    for halo in (halo_rates, halo_precond):
        for k in range(count * count):
            receive(halo.at[k], base)
            base += 1
    for f, ref in enumerate((state, quadratic, history)):
        for s in range(count):
            fields_ref[f, s, 0:rows, :] = ref[s]
            receive(fields_ref.at[f, s], base, rows)
            base += 1
    base = 2 * count + 4
    for g in range(base):
        strips_ref[g, 0:rows, :] = strips_in[g]
        receive(strips_ref.at[g], g, rows, sources)
    single = [(fields_ref.at[0, s], rows) for s in range(count)]
    for k in range(2):
        for s in range(count):
            inject_ref[k, s] = blank
            single.append((inject_ref.at[k, s], 0))
    single.append((strips_ref.at[2 * count], rows))
    for k in range(2):
        inject_s[k] = blank
        single.append((inject_s.at[k], 0))
    for j, (target, at) in enumerate(single):
        for source, keep, _, far in sources:
            target[pl.ds(at + far, 1), :] = source[base + j // 2, pl.ds(j % 2, 1), :] * keep

    speed = strip_speed(vel, count, ext)
    strips = lambda g: strips_ref[g]

    def put(k):
        def store(s, value):
            if s is None:
                vs_ref[k] = value
            else:
                v_ref[k, s] = value
        return store

    fields = [[fields_ref[f, s] for s in range(count)] for f in range(3)]
    first_vector(fields, rates, halo_rates, strips, vel, speed, put(0))

    far_row = (row_of(8) == 2) | (row_of(8) == 5)

    def patch(value, inject):
        return jnp.concatenate(
            [value[:rows], jnp.where(far_row, inject, value[rows:])], axis=0
        )

    for k in range(KRYLOV):
        pick = min(k, 1)
        v = [v_ref[k, s] for s in range(count)]
        for s in range(count):
            value = patch(row_product(precond, halo_precond, v, s), inject_ref[pick, s])
            zx_ref[s] = value
            z_out[k, s] = value[:rows]
        v_s = vs_ref[k]
        z_s = strip_product(lambda t: strips_ref[count + t], v_s, count)
        zs_ref[...] = patch(z_s, inject_s[pick])
        z = [zx_ref[s] for s in range(count)]
        apply_shifted(
            v, v_s, z, zs_ref,
            lambda s: 2.0 * fields_ref[1, s] * fields_ref[0, s],
            2.0 * strips_ref[2 * count + 1] * strips_ref[2 * count],
            rates, halo_rates, strips, vel, speed, put(k + 1),
        )

    pairs = pairs_of(KRYLOV + 1)

    def gather(s, carry):
        high, low = list(carry[0]), list(carry[1])
        for r in range(0, rows, 8):
            whole = [v_ref[k, s, r : r + 8, :] for k in range(KRYLOV + 1)]
            parts = [split(x) for x in whole]
            for n, (i, j) in enumerate(pairs):
                product = parts[i][0] * parts[j][0]
                rest = parts[i][0] * parts[j][1] + parts[i][1] * whole[j]
                high[n], error = two_sum(high[n], product)
                low[n] = low[n] + (error + rest)
        return tuple(high), tuple(low)

    zeros = tuple(blank for _ in pairs)
    high, low = lax.fori_loop(0, count, gather, (zeros, zeros))

    def fold(h, l, shift, move):
        h, error = two_sum(h, move(h, shift))
        return h, l + move(l, shift) + error

    row16, lane16 = row_of(16), lane_of(16)
    top = jnp.zeros((16, LANES), F32)
    bottom = jnp.zeros((16, LANES), F32)
    for n in range(len(pairs)):
        h, l = high[n], low[n]
        for shift in (4, 2, 1):
            h, l = fold(h, l, shift, roll_rows)
        top = jnp.where(row16 == n, jnp.concatenate([h, h], axis=0), top)
        bottom = jnp.where(row16 == n, jnp.concatenate([l, l], axis=0), bottom)
    for shift in (64, 32, 16, 8, 4, 2, 1):
        top, bottom = fold(top, bottom, shift, roll_lanes)
    top, bottom = quick_sum(top, bottom)
    bottom = roll_lanes(bottom, 16)
    line = jnp.where(row16 == lane16, top, 0.0) + jnp.where(row16 + 16 == lane16, bottom, 0.0)
    line = line[:8] + line[8:]
    for shift in (4, 2, 1):
        line = line + roll_rows(line, shift)
    for r in range(0, gram_out.shape[0], 8):
        gram_out[r : r + 8, :] = line


def small_problem(gram):
    width = KRYLOV + 1
    work = dict(gram)
    unit = {}
    pivot = []
    for k in range(width):
        dh, dl = work[k, k]
        pivot.append(jnp.maximum(dh, 0.0))
        inverse = jnp.where(dh > 0.0, 1.0 / jnp.where(dh > 0.0, dh, 1.0), 0.0)
        factor = {}
        for i in range(k + 1, width):
            sh, sl = work[k, i]
            q = sh * inverse
            p, e = two_prod(q, dh)
            rest = ((sh - p) - e) + (sl - q * dl)
            factor[i] = quick_sum(q, rest * inverse)
            unit[k, i] = factor[i][0]
        for i in range(k + 1, width):
            for j in range(i, width):
                fh, fl = factor[i]
                sh, sl = work[k, j]
                p, e = two_prod(fh, sh)
                e = e + (fh * sl + fl * sh)
                wh, wl = work[i, j]
                h, error = two_sum(wh, -p)
                work[i, j] = quick_sum(h, error + (wl - e))
    norm = [jnp.sqrt(d) for d in pivot]
    back = [jnp.where(n > 0.0, 1.0 / jnp.where(n > 0.0, n, 1.0), 0.0) for n in norm]
    inv = {}
    for j in range(KRYLOV):
        column = {j: None}
        inv[j, j] = back[j]
        for i in reversed(range(j)):
            total = unit[i, j] * back[j]
            for m in range(i + 1, j):
                total = total + unit[i, m] * inv[m, j]
            inv[i, j] = -total
    arnoldi = {}
    for j in range(KRYLOV):
        shifted = [inv[0, j]]
        for i in range(1, j + 1):
            shifted.append(inv[i, j] + inv[i - 1, j])
        shifted.append(inv[j, j])
        for i in range(j + 2):
            total = shifted[i]
            for m in range(i + 1, j + 2):
                total = total + unit[i, m] * shifted[m]
            arnoldi[i, j] = norm[i] * total
    beta = jnp.sqrt(pivot[0] + tiny_eps)
    basis = [[norm[0] / beta]]
    hessen = {}
    for k in range(KRYLOV):
        vector = []
        for i in range(k + 2):
            terms = [arnoldi[i, j] * basis[k][j] for j in range(max(i - 1, 0), k + 1)]
            vector.append(functools.reduce(jnp.add, terms))
        for i in range(k + 1):
            terms = [a * b for a, b in zip(basis[i], vector)]
            hessen[i, k] = functools.reduce(jnp.add, terms)
        for m in range(k + 1):
            terms = [hessen[i, k] * basis[i][m] for i in range(m, k + 1)]
            vector[m] = vector[m] - functools.reduce(jnp.add, terms)
        squared = functools.reduce(jnp.add, [x * x for x in vector])
        size = jnp.sqrt(squared + tiny_eps)
        hessen[k + 1, k] = size
        basis.append([x / size for x in vector])
    rotated = [beta] + [jnp.zeros_like(beta)] * KRYLOV
    for k in range(KRYLOV):
        first, second = hessen[k, k], hessen[k + 1, k]
        radius = jnp.sqrt(first * first + second * second)
        cosine, sine = first / radius, second / radius
        for j in range(k, KRYLOV):
            upper = hessen[k, j]
            under = hessen.get((k + 1, j))
            hessen[k, j] = cosine * upper + sine * under
            hessen[k + 1, j] = cosine * under - sine * upper
        rotated[k], rotated[k + 1] = (
            cosine * rotated[k] + sine * rotated[k + 1],
            cosine * rotated[k + 1] - sine * rotated[k],
        )
    coef = [None] * KRYLOV
    for k in reversed(range(KRYLOV)):
        total = rotated[k]
        for j in range(k + 1, KRYLOV):
            total = total - hessen[k, j] * coef[j]
        coef[k] = total / hessen[k, k]
    in_q = [
        functools.reduce(jnp.add, [coef[k] * basis[k][m] for k in range(m, KRYLOV)])
        for m in range(KRYLOV)
    ]
    in_v = [
        functools.reduce(jnp.add, [inv[i, j] * in_q[j] for j in range(i, KRYLOV)])
        for i in range(KRYLOV)
    ]
    return in_v, jnp.abs(rotated[KRYLOV])


def solve_kernel(gathered, z_ref, state, updated, residual):
    count, rows, _ = state.shape
    high = gathered[0:8, :]
    low = roll_lanes(high, -16)
    for r in range(8, gathered.shape[0], 8):
        tile = gathered[r : r + 8, :]
        high, error = two_sum(high, tile)
        low = low + roll_lanes(tile, -16) + error
    for shift in (4, 2, 1):
        high, error = two_sum(high, roll_rows(high, shift))
        low = low + roll_rows(low, shift) + error
    high, low = quick_sum(high, low)
    gram = {}
    for n, pair in enumerate(pairs_of(KRYLOV + 1)):
        gram[pair] = (
            jnp.broadcast_to(high[:, n : n + 1], (8, LANES)),
            jnp.broadcast_to(low[:, n : n + 1], (8, LANES)),
        )
    weights, last = small_problem(gram)
    for s in range(count):
        for r in range(0, rows, 8):
            total = weights[0] * z_ref[0, s, r : r + 8, :]
            for k in range(1, KRYLOV):
                total = total + weights[k] * z_ref[k, s, r : r + 8, :]
            updated[s, r : r + 8, :] = state[s, r : r + 8, :] + total
    residual[0] = last[0, 0]


def shapes(*dims):
    return jax.ShapeDtypeStruct(dims, F32)


def body(state, history, rates, quadratic, velocity, precond):
    count, rows, _ = state.shape
    part_count = lax.axis_size("parts")
    row_count = lax.axis_size("row")
    col_count = lax.axis_size("col")
    flip = part_count % 2 == 0
    block = (count, rows, LANES)

    square = (count,) + block
    smem = pl.BlockSpec(memory_space=pltpu.SMEM)
    whole = pl.BlockSpec(memory_space=pltpu.VMEM)
    inputs = [
        pltpu.with_memory_space_constraint(x, pltpu.HBM)
        for x in (state, history, rates, quadratic, precond)
    ]
    (
        state, history, rates, quadratic, precond, to_right, to_left, send_a, send_b
    ) = pl.pallas_call(
        functools.partial(pack_kernel, flip=flip),
        in_specs=[pl.BlockSpec(memory_space=pltpu.HBM)] * 5,
        out_shape=[
            shapes(*block), shapes(*block), shapes(*square), shapes(*block), shapes(*square),
            shapes(count + 2, rows, LANES), shapes(count + 2, rows, LANES),
            shapes(raw_planes(count), 2, LANES), shapes(raw_planes(count), 2, LANES),
        ],
        out_specs=[whole] * 9,
        scratch_shapes=[pltpu.SemaphoreType.DMA((5,))],
        compiler_params=VMEM,
        name="pack_columns",
    )(*inputs)
    ring = [(i, (i + 1) % col_count) for i in range(col_count)]
    from_left = lax.ppermute(to_right, "col", ring)
    from_right = lax.ppermute(to_left, "col", [(b, a) for a, b in ring])

    chain = []
    for p in range(part_count):
        for r in range(row_count):
            if flip and p % 2:
                target = (p, r - 1) if r else (p - 1, 0)
            elif flip:
                target = (p, r + 1) if r < row_count - 1 else (p + 1, r)
            else:
                target = (p, (r + 1) % row_count)
            chain.append((p * row_count + r, target[0] * row_count + target[1]))
    back = [(b, a) for a, b in chain]
    raw_a = lax.ppermute(send_a, ("parts", "row"), chain)
    raw_b = lax.ppermute(send_b, ("parts", "row"), back)

    planes = message_planes(count)
    strips, send_a, send_b = pl.pallas_call(
        functools.partial(half_kernel, counts=(col_count, flip)),
        in_specs=[whole] * 7 + [smem],
        out_shape=[shapes(2 * count + 4, rows, LANES)] + [shapes(planes, 2, LANES)] * 2,
        scratch_shapes=[
            pltpu.VMEM((2,) + block, F32),
            pltpu.VMEM((2,) + block, F32),
            pltpu.VMEM((2, rows, LANES), F32),
            pltpu.VMEM((2, rows, LANES), F32),
        ],
        compiler_params=VMEM,
        name="half_step",
    )(from_left, from_right, state, history, rates, quadratic, precond, velocity)

    got_a = lax.ppermute(send_a, ("parts", "row"), chain)
    got_b = lax.ppermute(send_b, ("parts", "row"), back)

    ext = rows + 8
    members = row_count * col_count
    z, gram = pl.pallas_call(
        functools.partial(full_kernel, row_count=row_count, flip=flip),
        in_specs=[whole] * 10 + [smem],
        out_shape=[shapes(KRYLOV, *block), shapes(members, LANES)],
        scratch_shapes=[
            pltpu.VMEM((count * count, 8, LANES), F32),
            pltpu.VMEM((count * count, 8, LANES), F32),
            pltpu.VMEM((3, count, ext, LANES), F32),
            pltpu.VMEM((2 * count + 4, ext, LANES), F32),
            pltpu.VMEM((2, count, 8, LANES), F32),
            pltpu.VMEM((2, 8, LANES), F32),
            pltpu.VMEM((KRYLOV + 1, count, ext, LANES), F32),
            pltpu.VMEM((KRYLOV + 1, ext, LANES), F32),
            pltpu.VMEM((count, ext, LANES), F32),
            pltpu.VMEM((ext, LANES), F32),
        ],
        compiler_params=VMEM,
        name="krylov",
    )(raw_a, raw_b, got_a, got_b, strips, state, history, rates, quadratic, precond, velocity)

    gathered = lax.all_to_all(gram, ("row", "col"), 0, 0, tiled=True)
    updated, last = pl.pallas_call(
        solve_kernel,
        out_shape=[shapes(*block), shapes(1)],
        out_specs=[whole, smem],
        compiler_params=VMEM,
        name="solve",
    )(gathered, z, state)
    return updated, last


def solution(mesh):
    placed = (
        P(None, ("parts", "row"), "col"),
        P(None, ("parts", "row"), "col"),
        P(None, None, ("parts", "row"), "col"),
        P(None, ("parts", "row"), "col"),
        P(),
        P(None, None, ("parts", "row"), "col"),
    )
    return jax.shard_map(
        body,
        mesh=mesh,
        in_specs=placed,
        out_specs=(P(None, ("parts", "row"), "col"), P("parts")),
        check_vma=False,
    )
```

```python
import functools

import jax
import jax.numpy as jnp
from jax import lax
from jax.experimental import pallas as pl
from jax.experimental.pallas import tpu as pltpu
from jax.sharding import PartitionSpec as P

KRYLOV = 4
step_gamma = 0.4
tiny_eps = 1e-12

F32 = jnp.float32
LANES = 128
VMEM = pltpu.CompilerParams(vmem_limit_bytes=48 * 1024 * 1024)


def lane_of(rows):
    return lax.broadcasted_iota(jnp.int32, (rows, LANES), 1)


def row_of(rows):
    return lax.broadcasted_iota(jnp.int32, (rows, LANES), 0)


def roll_lanes(x, shift):
    shift %= LANES
    return pltpu.roll(x, shift, 1) if shift else x


def roll_rows(x, shift):
    return pltpu.roll(x, shift % x.shape[0], 0)


def slot_of(rows):
    return ((131 - lane_of(rows)) // 8) % 16


def two_sum(a, b):
    s = a + b
    t = s - a
    return s, (a - (s - t)) + (b - t)


def quick_sum(a, b):
    s = a + b
    return s, b - (s - a)


def split(a):
    c = a * 4097.0
    high = c - (c - a)
    return high, a - high


def two_prod(a, b):
    p = a * b
    ah, al = split(a)
    bh, bl = split(b)
    return p, ((ah * bh - p) + ah * bl + al * bh) + al * bl


def move_main(main, strip, s):
    lane = lane_of(main.shape[0])
    left = jnp.where(lane == 0, roll_lanes(strip, 8 * s + 1), roll_lanes(main, 1))
    right = jnp.where(lane == LANES - 1, roll_lanes(strip, 8 * s - 1), roll_lanes(main, -1))
    return left, right


def move_strip(mains, strip, second=None):
    rows = strip.shape[0]
    lane = lane_of(rows)
    slot = slot_of(rows)
    edge = jnp.zeros((rows, LANES), F32)
    for s, main in enumerate(mains):
        both = jnp.where(
            lane % 8 == 7, roll_lanes(main, -(8 * s + 1)), roll_lanes(main, 1 - 8 * s)
        )
        edge = jnp.where(slot == s, both, edge)
    left = jnp.where(lane % 8 == 0, edge, roll_lanes(strip, 1))
    right = jnp.where(lane % 8 == 7, edge, roll_lanes(strip, -1))
    if second is not None:
        left = jnp.where(lane % 8 == 4, roll_lanes(second, -3), left)
        right = jnp.where(lane % 8 == 3, roll_lanes(second, 3), right)
    return left, right


def drift(field, left, right, vx, vy):
    along_x = roll_rows(field, -1) - roll_rows(field, 1)
    return -0.5 * (vx * along_x + vy * (right - left))


def speeds(vel, count, rows):
    slot = slot_of(rows)
    mains = [
        tuple(jnp.broadcast_to(vel[s : s + 1, d : d + 1], (rows, LANES)) for d in range(2))
        for s in range(count)
    ]
    strip = [jnp.zeros((rows, LANES), F32)] * 2
    for s in range(count):
        strip = [jnp.where(slot == s, x, y) for x, y in zip(mains[s], strip)]
    return mains, strip


def spread(strip, t):
    lane = lane_of(strip.shape[0])
    source = (LANES - 4 - 8 * t + (lane + 4) % 8) % LANES
    return jnp.take_along_axis(strip, source, axis=1)


def strip_product(get, strip, count):
    total = get(0) * spread(strip, 0)
    for t in range(1, count):
        total = total + get(t) * spread(strip, t)
    return total


def row_product(block, halo, mains, s):
    count = len(mains)
    rows = block.shape[2]
    total = block[s, 0] * mains[0][:rows]
    for t in range(1, count):
        total = total + block[s, t] * mains[t][:rows]
    if halo is None:
        return total
    extra = halo[s * count] * mains[0][rows:]
    for t in range(1, count):
        extra = extra + halo[s * count + t] * mains[t][rows:]
    return jnp.concatenate([total, extra], axis=0)


def first_vector(fields, rates, halo_rates, strips, vel, speed, store):
    state, quad, hist = fields
    count = len(state)
    state_s, quad_s, hist_s, second = strips(2 * count), strips(2 * count + 1), strips(
        2 * count + 2
    ), strips(2 * count + 3)
    for s in range(count):
        left, right = move_main(state[s], state_s, s)
        forcing = drift(state[s], left, right, *vel[s])
        forcing = forcing + row_product(rates, halo_rates, state, s)
        forcing = forcing - quad[s] * state[s] * state[s]
        store(s, -(state[s] - hist[s] - step_gamma * forcing))
    left, right = move_strip(state, state_s, second)
    forcing = drift(state_s, left, right, *speed)
    forcing = forcing + strip_product(strips, state_s, count)
    forcing = forcing - quad_s * state_s * state_s
    store(None, -(state_s - hist_s - step_gamma * forcing))


def apply_shifted(v, v_s, z, z_s, damp, damp_s, rates, halo_rates, strips, vel, speed, store):
    count = len(z)
    for s in range(count):
        left, right = move_main(z[s], z_s[...], s)
        jac = drift(z[s], left, right, *vel[s])
        jac = jac + row_product(rates, halo_rates, z, s) - damp(s) * z[s]
        store(s, (z[s] - step_gamma * jac) - v[s])
    z_s = z_s[...]
    left, right = move_strip(z, z_s)
    jac = drift(z_s, left, right, *speed)
    jac = jac + strip_product(strips, z_s, count) - damp_s * z_s
    store(None, (z_s - step_gamma * jac) - v_s)


def edge_rows(rows, flip):
    odd = (lax.axis_index("parts") % 2) if flip else 0
    down, up = (rows - 2, rows - 3), (0, 2)
    return tuple(
        tuple(x + (y - x) * odd for x, y in zip(*ends)) for ends in ((down, up), (up, down))
    )


def pack_kernel(
    state_in, history_in, rates_in, quadratic_in, precond_in,
    state, history, rates, quadratic, precond, to_right, to_left, raw_a, raw_b, sems, *, flip,
):
    count, rows, _ = state.shape
    copies = [
        pltpu.make_async_copy(source, target, sems.at[n])
        for n, (source, target) in enumerate(
            (
                (rates_in, rates),
                (precond_in, precond),
                (state_in, state),
                (quadratic_in, quadratic),
                (history_in, history),
            )
        )
    ]
    for copy in copies:
        copy.start()
    slot = slot_of(rows)
    low = lane_of(rows) % 8 < 4

    def group(index):
        packed = jnp.zeros((rows, LANES), F32)
        for s in range(count):
            if index < count:
                plane = rates[s, index]
            elif index < 2 * count:
                plane = precond[s, index - count]
            else:
                plane = (state, quadratic, history, state)[index - 2 * count][s]
            if index == 2 * count + 3:
                moved = jnp.where(
                    low, roll_lanes(plane, -4 - 8 * s), roll_lanes(plane, 4 - 8 * s)
                )
            else:
                moved = roll_lanes(plane, -8 * s)
            packed = jnp.where(slot == s, moved, packed)
        return packed

    done = set()
    for pair in range(count + 2):
        ready = 1 if 2 * pair + 1 < count else 2 if 2 * pair + 1 < 2 * count else 5
        for n in range(ready):
            if n not in done:
                copies[n].wait()
                done.add(n)
        one, two = group(2 * pair), group(2 * pair + 1)
        to_right[pair] = jnp.where(low, roll_lanes(two, -4), one)
        to_left[pair] = jnp.where(low, one, roll_lanes(two, 4))

    for target, (near, _) in zip((raw_a, raw_b), edge_rows(rows, flip)):
        planes = [m.at[s, t] for m in (rates, precond) for s in range(count) for t in range(count)]
        planes += [ref.at[s] for ref in (state, quadratic, history) for s in range(count)]
        for n, ref in enumerate(planes):
            target[n] = ref[pl.ds(near, 2), :]


def half_kernel(
    from_left, from_right, state, history, rates, quadratic, precond, vel,
    strips_out, send_a, send_b, v_ref, z_ref, vs_ref, zs_ref, *, counts,
):
    count, rows, _ = state.shape
    cols, flip = counts
    low = lane_of(rows) % 8 < 4
    position = lax.axis_index("col")
    has_left = (position > 0).astype(F32)
    has_right = (position < cols - 1).astype(F32)
    for pair in range(count + 2):
        left = from_left[pair] * has_left
        right = from_right[pair] * has_right
        strips_out[2 * pair] = jnp.where(low, right, left)
        strips_out[2 * pair + 1] = jnp.where(low, roll_lanes(right, -4), roll_lanes(left, 4))

    vel, speed = speeds(vel, count, rows)
    strips = lambda g: strips_out[g]
    fields = [[ref[s] for s in range(count)] for ref in (state, quadratic, history)]

    def put(k):
        def store(s, value):
            if s is None:
                vs_ref[k] = value
            else:
                v_ref[k, s] = value

        return store

    def precondition(k):
        v = [v_ref[k, s] for s in range(count)]
        for s in range(count):
            z_ref[k, s] = row_product(precond, None, v, s)
        zs_ref[k] = strip_product(lambda t: strips_out[count + t], vs_ref[k], count)

    first_vector(fields, rates, None, strips, vel, speed, put(0))
    precondition(0)
    apply_shifted(
        [v_ref[0, s] for s in range(count)], vs_ref[0],
        [z_ref[0, s] for s in range(count)], zs_ref.at[0],
        lambda s: 2.0 * quadratic[s] * state[s],
        2.0 * strips_out[2 * count + 1] * strips_out[2 * count],
        rates, None, strips, vel, speed, put(1),
    )
    precondition(1)

    single = [state.at[s] for s in range(count)]
    single += [z_ref.at[k, s] for k in range(2) for s in range(count)]
    single += [strips_out.at[2 * count], zs_ref.at[0], zs_ref.at[1]]
    base = 2 * count + 4
    for target, (near, far) in zip((send_a, send_b), edge_rows(rows, flip)):
        for g in range(base):
            target[g] = strips_out[g, pl.ds(near, 2), :]
        for j, ref in enumerate(single):
            target[base + j // 2, pl.ds(j % 2, 1), :] = ref[pl.ds(far, 1), :]
        if len(single) % 2:
            target[base + len(single) // 2, pl.ds(1, 1), :] = jnp.zeros((1, LANES), F32)


def raw_planes(count):
    return 2 * count * count + 3 * count


def message_planes(count):
    return (2 * count + 4) + (3 * count + 3 + 1) // 2


def pairs_of(width):
    return [(i, j) for i in range(width) for j in range(i, width)]


def full_kernel(
    raw_a, raw_b, got_a, got_b, strips_in, state, history, rates, quadratic, precond, vel,
    z_out, gram_out,
    halo_rates, halo_precond, fields_ref, strips_ref, inject_ref, inject_s, v_ref, vs_ref,
    zx_ref, zs_ref, *, row_count, flip,
):
    count, rows, _ = state.shape
    ext = rows + 8
    odd = (lax.axis_index("parts") % 2) if flip else 0
    position = lax.axis_index("row")
    above = (position > 0).astype(F32)
    below = (position < row_count - 1).astype(F32)
    odd_f = jnp.asarray(odd).astype(F32)
    keep_a = above * (1 - odd_f) + below * odd_f
    keep_b = below * (1 - odd_f) + above * odd_f
    near_a, far_a = 6 * (1 - odd), 5 * (1 - odd) + 2 * odd
    near_b, far_b = 6 * odd, 5 * odd + 2 * (1 - odd)
    raws = ((raw_a, keep_a, near_a), (raw_b, keep_b, near_b))
    sources = ((got_a, keep_a, near_a, far_a), (got_b, keep_b, near_b, far_b))
    blank = jnp.zeros((8, LANES), F32)

    def receive(target, base, at=0, sources=raws):
        target[pl.ds(at, 8), :] = blank
        for source, keep, near, *_ in sources:
            target[pl.ds(at + near, 2), :] = source[base] * keep

    base = 0
    for halo in (halo_rates, halo_precond):
        for k in range(count * count):
            receive(halo.at[k], base)
            base += 1
    for f, ref in enumerate((state, quadratic, history)):
        for s in range(count):
            fields_ref[f, s, 0:rows, :] = ref[s]
            receive(fields_ref.at[f, s], base, rows)
            base += 1
    base = 2 * count + 4
    for g in range(base):
        strips_ref[g, 0:rows, :] = strips_in[g]
        receive(strips_ref.at[g], g, rows, sources)
    single = [(fields_ref.at[0, s], rows) for s in range(count)]
    for k in range(2):
        for s in range(count):
            inject_ref[k, s] = blank
            single.append((inject_ref.at[k, s], 0))
    single.append((strips_ref.at[2 * count], rows))
    for k in range(2):
        inject_s[k] = blank
        single.append((inject_s.at[k], 0))
    for j, (target, at) in enumerate(single):
        for source, keep, _, far in sources:
            target[pl.ds(at + far, 1), :] = source[base + j // 2, pl.ds(j % 2, 1), :] * keep

    vel, speed = speeds(vel, count, ext)
    strips = lambda g: strips_ref[g]

    def put(k):
        def store(s, value):
            if s is None:
                vs_ref[k] = value
            else:
                v_ref[k, s] = value

        return store

    fields = [[fields_ref[f, s] for s in range(count)] for f in range(3)]
    first_vector(fields, rates, halo_rates, strips, vel, speed, put(0))

    far_row = (row_of(8) == 2) | (row_of(8) == 5)

    def patch(value, inject):
        return jnp.concatenate(
            [value[:rows], jnp.where(far_row, inject, value[rows:])], axis=0
        )

    for k in range(KRYLOV):
        pick = min(k, 1)
        v = [v_ref[k, s] for s in range(count)]
        for s in range(count):
            value = patch(row_product(precond, halo_precond, v, s), inject_ref[pick, s])
            zx_ref[s] = value
            z_out[k, s] = value[:rows]
        v_s = vs_ref[k]
        z_s = strip_product(lambda t: strips_ref[count + t], v_s, count)
        zs_ref[...] = patch(z_s, inject_s[pick])
        z = [zx_ref[s] for s in range(count)]
        apply_shifted(
            v, v_s, z, zs_ref,
            lambda s: 2.0 * fields_ref[1, s] * fields_ref[0, s],
            2.0 * strips_ref[2 * count + 1] * strips_ref[2 * count],
            rates, halo_rates, strips, vel, speed, put(k + 1),
        )

    pairs = pairs_of(KRYLOV + 1)

    def gather(s, carry):
        high, low = list(carry[0]), list(carry[1])
        for r in range(0, rows, 8):
            whole = [v_ref[k, s, r : r + 8, :] for k in range(KRYLOV + 1)]
            parts = [split(x) for x in whole]
            for n, (i, j) in enumerate(pairs):
                product = parts[i][0] * parts[j][0]
                rest = parts[i][0] * parts[j][1] + parts[i][1] * whole[j]
                high[n], error = two_sum(high[n], product)
                low[n] = low[n] + (error + rest)
        return tuple(high), tuple(low)

    zeros = tuple(blank for _ in pairs)
    high, low = lax.fori_loop(0, count, gather, (zeros, zeros))

    def fold(h, l, shift, move):
        h, error = two_sum(h, move(h, shift))
        return h, l + move(l, shift) + error

    row16, lane16 = row_of(16), lane_of(16)
    top = jnp.zeros((16, LANES), F32)
    bottom = jnp.zeros((16, LANES), F32)
    for n in range(len(pairs)):
        h, l = high[n], low[n]
        for shift in (4, 2, 1):
            h, l = fold(h, l, shift, roll_rows)
        top = jnp.where(row16 == n, jnp.concatenate([h, h], axis=0), top)
        bottom = jnp.where(row16 == n, jnp.concatenate([l, l], axis=0), bottom)
    for shift in (64, 32, 16, 8, 4, 2, 1):
        top, bottom = fold(top, bottom, shift, roll_lanes)
    top, bottom = quick_sum(top, bottom)
    bottom = roll_lanes(bottom, 16)
    line = jnp.where(row16 == lane16, top, 0.0) + jnp.where(row16 + 16 == lane16, bottom, 0.0)
    line = line[:8] + line[8:]
    for shift in (4, 2, 1):
        line = line + roll_rows(line, shift)
    for r in range(0, gram_out.shape[0], 8):
        gram_out[r : r + 8, :] = line


def small_problem(gram):
    width = KRYLOV + 1
    work = dict(gram)
    unit = {}
    pivot = []
    for k in range(width):
        dh, dl = work[k, k]
        pivot.append(jnp.maximum(dh, 0.0))
        inverse = jnp.where(dh > 0.0, 1.0 / jnp.where(dh > 0.0, dh, 1.0), 0.0)
        factor = {}
        for i in range(k + 1, width):
            sh, sl = work[k, i]
            q = sh * inverse
            p, e = two_prod(q, dh)
            rest = ((sh - p) - e) + (sl - q * dl)
            factor[i] = quick_sum(q, rest * inverse)
            unit[k, i] = factor[i][0]
        for i in range(k + 1, width):
            for j in range(i, width):
                fh, fl = factor[i]
                sh, sl = work[k, j]
                p, e = two_prod(fh, sh)
                e = e + (fh * sl + fl * sh)
                wh, wl = work[i, j]
                h, error = two_sum(wh, -p)
                work[i, j] = quick_sum(h, error + (wl - e))
    norm = [jnp.sqrt(d) for d in pivot]
    back = [jnp.where(n > 0.0, 1.0 / jnp.where(n > 0.0, n, 1.0), 0.0) for n in norm]
    inv = {}
    for j in range(KRYLOV):
        inv[j, j] = back[j]
        for i in reversed(range(j)):
            total = unit[i, j] * back[j]
            for m in range(i + 1, j):
                total = total + unit[i, m] * inv[m, j]
            inv[i, j] = -total
    arnoldi = {}
    for j in range(KRYLOV):
        shifted = [inv[0, j]]
        for i in range(1, j + 1):
            shifted.append(inv[i, j] + inv[i - 1, j])
        shifted.append(inv[j, j])
        for i in range(j + 2):
            total = shifted[i]
            for m in range(i + 1, j + 2):
                total = total + unit[i, m] * shifted[m]
            arnoldi[i, j] = norm[i] * total
    beta = jnp.sqrt(pivot[0] + tiny_eps)
    basis = [[norm[0] / beta]]
    hessen = {}
    for k in range(KRYLOV):
        vector = []
        for i in range(k + 2):
            terms = [arnoldi[i, j] * basis[k][j] for j in range(max(i - 1, 0), k + 1)]
            vector.append(functools.reduce(jnp.add, terms))
        for i in range(k + 1):
            terms = [a * b for a, b in zip(basis[i], vector)]
            hessen[i, k] = functools.reduce(jnp.add, terms)
        for m in range(k + 1):
            terms = [hessen[i, k] * basis[i][m] for i in range(m, k + 1)]
            vector[m] = vector[m] - functools.reduce(jnp.add, terms)
        squared = functools.reduce(jnp.add, [x * x for x in vector])
        size = jnp.sqrt(squared + tiny_eps)
        hessen[k + 1, k] = size
        basis.append([x / size for x in vector])
    rotated = [beta] + [jnp.zeros_like(beta)] * KRYLOV
    for k in range(KRYLOV):
        first, second = hessen[k, k], hessen[k + 1, k]
        radius = jnp.sqrt(first * first + second * second)
        cosine, sine = first / radius, second / radius
        for j in range(k, KRYLOV):
            upper = hessen[k, j]
            under = hessen.get((k + 1, j))
            hessen[k, j] = cosine * upper + sine * under
            hessen[k + 1, j] = cosine * under - sine * upper
        rotated[k], rotated[k + 1] = (
            cosine * rotated[k] + sine * rotated[k + 1],
            cosine * rotated[k + 1] - sine * rotated[k],
        )
    coef = [None] * KRYLOV
    for k in reversed(range(KRYLOV)):
        total = rotated[k]
        for j in range(k + 1, KRYLOV):
            total = total - hessen[k, j] * coef[j]
        coef[k] = total / hessen[k, k]
    in_q = [
        functools.reduce(jnp.add, [coef[k] * basis[k][m] for k in range(m, KRYLOV)])
        for m in range(KRYLOV)
    ]
    in_v = [
        functools.reduce(jnp.add, [inv[i, j] * in_q[j] for j in range(i, KRYLOV)])
        for i in range(KRYLOV)
    ]
    return in_v, jnp.abs(rotated[KRYLOV])


def solve_kernel(gathered, z_ref, state, updated, residual):
    count, rows, _ = state.shape
    high = gathered[0:8, :]
    low = roll_lanes(high, -16)
    for r in range(8, gathered.shape[0], 8):
        tile = gathered[r : r + 8, :]
        high, error = two_sum(high, tile)
        low = low + roll_lanes(tile, -16) + error
    for shift in (4, 2, 1):
        high, error = two_sum(high, roll_rows(high, shift))
        low = low + roll_rows(low, shift) + error
    high, low = quick_sum(high, low)
    gram = {}
    for n, pair in enumerate(pairs_of(KRYLOV + 1)):
        gram[pair] = (
            jnp.broadcast_to(high[:, n : n + 1], (8, LANES)),
            jnp.broadcast_to(low[:, n : n + 1], (8, LANES)),
        )
    weights, last = small_problem(gram)
    for s in range(count):
        for r in range(0, rows, 8):
            total = weights[0] * z_ref[0, s, r : r + 8, :]
            for k in range(1, KRYLOV):
                total = total + weights[k] * z_ref[k, s, r : r + 8, :]
            updated[s, r : r + 8, :] = state[s, r : r + 8, :] + total
    residual[0] = last[0, 0]


def shapes(*dims):
    return jax.ShapeDtypeStruct(dims, F32)


def body(state, history, rates, quadratic, velocity, precond):
    count, rows, _ = state.shape
    part_count = lax.axis_size("parts")
    row_count = lax.axis_size("row")
    col_count = lax.axis_size("col")
    flip = part_count % 2 == 0
    block = (count, rows, LANES)

    square = (count,) + block
    smem = pl.BlockSpec(memory_space=pltpu.SMEM)
    whole = pl.BlockSpec(memory_space=pltpu.VMEM)
    inputs = [
        pltpu.with_memory_space_constraint(x, pltpu.HBM)
        for x in (state, history, rates, quadratic, precond)
    ]
    (
        state, history, rates, quadratic, precond, to_right, to_left, send_a, send_b
    ) = pl.pallas_call(
        functools.partial(pack_kernel, flip=flip),
        in_specs=[pl.BlockSpec(memory_space=pltpu.HBM)] * 5,
        out_shape=[
            shapes(*block), shapes(*block), shapes(*square), shapes(*block), shapes(*square),
            shapes(count + 2, rows, LANES), shapes(count + 2, rows, LANES),
            shapes(raw_planes(count), 2, LANES), shapes(raw_planes(count), 2, LANES),
        ],
        out_specs=[whole] * 9,
        scratch_shapes=[pltpu.SemaphoreType.DMA((5,))],
        compiler_params=VMEM,
        name="pack_columns",
    )(*inputs)
    ring = [(i, (i + 1) % col_count) for i in range(col_count)]
    from_left = lax.ppermute(to_right, "col", ring)
    from_right = lax.ppermute(to_left, "col", [(b, a) for a, b in ring])

    chain = []
    for p in range(part_count):
        for r in range(row_count):
            if flip and p % 2:
                target = (p, r - 1) if r else (p - 1, 0)
            elif flip:
                target = (p, r + 1) if r < row_count - 1 else (p + 1, r)
            else:
                target = (p, (r + 1) % row_count)
            chain.append((p * row_count + r, target[0] * row_count + target[1]))
    back = [(b, a) for a, b in chain]
    raw_a = lax.ppermute(send_a, ("parts", "row"), chain)
    raw_b = lax.ppermute(send_b, ("parts", "row"), back)

    planes = message_planes(count)
    strips, send_a, send_b = pl.pallas_call(
        functools.partial(half_kernel, counts=(col_count, flip)),
        in_specs=[whole] * 8,
        out_shape=[shapes(2 * count + 4, rows, LANES)] + [shapes(planes, 2, LANES)] * 2,
        scratch_shapes=[
            pltpu.VMEM((2,) + block, F32),
            pltpu.VMEM((2,) + block, F32),
            pltpu.VMEM((2, rows, LANES), F32),
            pltpu.VMEM((2, rows, LANES), F32),
        ],
        compiler_params=VMEM,
        name="half_step",
    )(from_left, from_right, state, history, rates, quadratic, precond, velocity)

    got_a = lax.ppermute(send_a, ("parts", "row"), chain)
    got_b = lax.ppermute(send_b, ("parts", "row"), back)

    ext = rows + 8
    members = row_count * col_count
    z, gram = pl.pallas_call(
        functools.partial(full_kernel, row_count=row_count, flip=flip),
        in_specs=[whole] * 11,
        out_shape=[shapes(KRYLOV, *block), shapes(members, LANES)],
        scratch_shapes=[
            pltpu.VMEM((count * count, 8, LANES), F32),
            pltpu.VMEM((count * count, 8, LANES), F32),
            pltpu.VMEM((3, count, ext, LANES), F32),
            pltpu.VMEM((2 * count + 4, ext, LANES), F32),
            pltpu.VMEM((2, count, 8, LANES), F32),
            pltpu.VMEM((2, 8, LANES), F32),
            pltpu.VMEM((KRYLOV + 1, count, ext, LANES), F32),
            pltpu.VMEM((KRYLOV + 1, ext, LANES), F32),
            pltpu.VMEM((count, ext, LANES), F32),
            pltpu.VMEM((ext, LANES), F32),
        ],
        compiler_params=VMEM,
        name="krylov",
    )(raw_a, raw_b, got_a, got_b, strips, state, history, rates, quadratic, precond, velocity)

    gathered = lax.all_to_all(gram, ("row", "col"), 0, 0, tiled=True)
    updated, last = pl.pallas_call(
        solve_kernel,
        out_shape=[shapes(*block), shapes(1)],
        out_specs=[whole, smem],
        compiler_params=VMEM,
        name="solve",
    )(gathered, z, state)
    return updated, last


def solution(mesh):
    placed = (
        P(None, ("parts", "row"), "col"),
        P(None, ("parts", "row"), "col"),
        P(None, None, ("parts", "row"), "col"),
        P(None, ("parts", "row"), "col"),
        P(),
        P(None, None, ("parts", "row"), "col"),
    )
    return jax.shard_map(
        body,
        mesh=mesh,
        in_specs=placed,
        out_specs=(P(None, ("parts", "row"), "col"), P("parts")),
        check_vma=False,
    )
```

```python
import functools

import jax
import jax.numpy as jnp
from jax import lax
from jax.experimental import pallas as pl
from jax.experimental.pallas import tpu as pltpu
from jax.sharding import PartitionSpec as P

KRYLOV = 4
step_gamma = 0.4
tiny_eps = 1e-12

F32 = jnp.float32
LANES = 128
VMEM = pltpu.CompilerParams(vmem_limit_bytes=48 * 1024 * 1024)


def lane_of(rows):
    return lax.broadcasted_iota(jnp.int32, (rows, LANES), 1)


def row_of(rows):
    return lax.broadcasted_iota(jnp.int32, (rows, LANES), 0)


def roll_lanes(x, shift):
    shift %= LANES
    return pltpu.roll(x, shift, 1) if shift else x


def roll_rows(x, shift):
    return pltpu.roll(x, shift % x.shape[0], 0)


def slot_of(rows):
    return ((131 - lane_of(rows)) // 8) % 16


def two_sum(a, b):
    s = a + b
    t = s - a
    return s, (a - (s - t)) + (b - t)


def quick_sum(a, b):
    s = a + b
    return s, b - (s - a)


def split(a):
    c = a * 4097.0
    high = c - (c - a)
    return high, a - high


def two_prod(a, b):
    p = a * b
    ah, al = split(a)
    bh, bl = split(b)
    return p, ((ah * bh - p) + ah * bl + al * bh) + al * bl


def tile_rows(n):
    return slice(8 * n, 8 * n + 8)


def vertical(field, n):
    tiles = field.shape[0] // 8
    this = field[tile_rows(n), :]
    following = field[tile_rows((n + 1) % tiles), :]
    leading = field[tile_rows((n - 1) % tiles), :]
    row = row_of(8)
    under = roll_rows(jnp.where(row == 0, following, this), -1)
    over = roll_rows(jnp.where(row == 7, leading, this), 1)
    return under - over


def speeds(vel, count):
    slot = slot_of(8)
    mains = [
        tuple(
            jnp.broadcast_to(0.5 * step_gamma * vel[s : s + 1, d : d + 1], (8, LANES))
            for d in range(2)
        )
        for s in range(count)
    ]
    strip = [jnp.zeros((8, LANES), F32)] * 2
    for s in range(count):
        strip = [jnp.where(slot == s, x, y) for x, y in zip(mains[s], strip)]
    return mains, strip


def diagonals(count):
    return range(-((count - 1) // 2), count // 2 + 1)


def sum_of(terms):
    return functools.reduce(jnp.add, terms)


def products(tile, fields):
    span = range(len(fields))
    return [sum_of([tile(s, t) * fields[t] for t in span]) for s in span]


def strip_product(strips, base, n, strip, count):
    slot = slot_of(8)
    past_end = jnp.where(slot < count, strip, roll_lanes(strip, -8 * count))
    past_start = jnp.where(slot < count, strip, roll_lanes(strip, -8 * (16 - count)))
    return sum_of(
        [
            strips[base + g, tile_rows(n), :] * roll_lanes(past_end if d >= 0 else past_start, 8 * d)
            for g, d in enumerate(diagonals(count))
        ]
    )


def drift(ring, ring_s, n, speed, count, second=None, with_strip=True):
    vel, vel_s = speed
    lane, slot = lane_of(8), slot_of(8)
    strip = ring_s[tile_rows(n), :]
    edge = jnp.zeros((8, LANES), F32)
    mains, moved = [], []
    for s in range(count):
        main = ring[s, tile_rows(n), :]
        outer = roll_lanes(strip, 8 * s)
        left = roll_lanes(jnp.where(lane == LANES - 1, outer, main), 1)
        right = roll_lanes(jnp.where(lane == 0, outer, main), -1)
        along_x = vertical(ring.at[s], n)
        moved.append(vel[s][0] * along_x + vel[s][1] * (right - left))
        if with_strip:
            edge = jnp.where(slot == s, roll_lanes(main, -8 * s), edge)
        mains.append(main)
    if not with_strip:
        return mains, strip, moved, None
    left = roll_lanes(jnp.where(lane % 8 == 7, edge, strip), 1)
    right = roll_lanes(jnp.where(lane % 8 == 0, edge, strip), -1)
    if second is not None:
        left = jnp.where(lane % 8 == 4, roll_lanes(second, -3), left)
        right = jnp.where(lane % 8 == 3, roll_lanes(second, 3), right)
    along_x = vertical(ring_s, n)
    return mains, strip, moved, vel_s[0] * along_x + vel_s[1] * (right - left)


def first_vector(n, state_ring, state_ring_s, quad, hist, rates, strips, speed, count, put, damp):
    base = 2 * count
    second = strips[base + 3, tile_rows(n), :]
    state, strip, moved, moved_s = drift(state_ring, state_ring_s, n, speed, count, second)
    linear = products(rates, state)
    for s in range(count):
        loss = step_gamma * quad(s) * state[s]
        damp(s, 1.0 + 2.0 * loss)
        put(s, ((hist(s) - state[s]) - moved[s]) + (step_gamma * linear[s] - loss * state[s]))
    linear = strip_product(strips, 0, n, strip, count)
    loss = step_gamma * strips[base + 1, tile_rows(n), :] * strip
    damp(None, 1.0 + 2.0 * loss)
    past = strips[base + 2, tile_rows(n), :]
    put(None, ((past - strip) - moved_s) + (step_gamma * linear - loss * strip))


def next_vector(n, ring, ring_s, old, rates, strips, speed, count, put, damp, with_strip=True):
    z, strip, moved, moved_s = drift(ring, ring_s, n, speed, count, None, with_strip)
    linear = products(rates, z)
    for s in range(count):
        put(s, ((damp(s) * z[s] - old(s)) + moved[s]) - step_gamma * linear[s])
    if with_strip:
        linear = strip_product(strips, 0, n, strip, count)
        put(None, ((damp(None) * strip - old(None)) + moved_s) - step_gamma * linear)


def odd_part(flip):
    return lax.axis_index("parts") % 2 if flip else jnp.int32(0)


def edge_rows(rows, flip):
    odd = odd_part(flip)
    down, up = (rows - 2, rows - 3), (0, 2)
    return tuple(
        tuple(x + (y - x) * odd for x, y in zip(*ends)) for ends in ((down, up), (up, down))
    )


def pack_kernel(
    state_in, history_in, rates_in, quadratic_in, precond_in,
    state, history, rates, quadratic, precond, edge_a, edge_b, raw_a, raw_b, sems, *, flip,
):
    count, rows, _ = state.shape
    copies = [
        pltpu.make_async_copy(source, target, sems.at[n])
        for n, (source, target) in enumerate(
            (
                (rates_in, rates),
                (precond_in, precond),
                (state_in, state),
                (quadratic_in, quadratic),
                (history_in, history),
            )
        )
    ]
    for copy in copies:
        copy.start()
    odd = odd_part(flip) == 1
    slot = slot_of(rows)
    low = lane_of(rows) % 8 < 4

    def group(index):
        packed = jnp.zeros((rows, LANES), F32)
        for s in range(count):
            if index < 2 * count:
                other = (s + diagonals(count)[index % count]) % count
                plane = (rates if index < count else precond)[s, other]
            else:
                plane = (state, quadratic, history, state)[index - 2 * count][s]
            if index == 2 * count + 3:
                moved = jnp.where(
                    low, roll_lanes(plane, -4 - 8 * s), roll_lanes(plane, 4 - 8 * s)
                )
            else:
                moved = roll_lanes(plane, -8 * s)
            packed = jnp.where(slot == s, moved, packed)
        return packed

    done = set()
    for pair in range(count + 2):
        ready = 1 if 2 * pair + 1 < count else 2 if 2 * pair + 1 < 2 * count else 5
        for n in range(ready):
            if n not in done:
                copies[n].wait()
                done.add(n)
        one, two = group(2 * pair), group(2 * pair + 1)
        right = jnp.where(low, roll_lanes(two, -4), one)
        left = jnp.where(low, one, roll_lanes(two, 4))
        edge_a[pair] = right
        edge_b[pair] = left

    for target, (near, _) in zip((raw_a, raw_b), edge_rows(rows, flip)):
        planes = [m.at[s, t] for m in (rates, precond) for s in range(count) for t in range(count)]
        planes += [ref.at[s] for ref in (state, quadratic, history) for s in range(count)]
        for n, ref in enumerate(planes):
            target[n] = ref[pl.ds(near, 2), :]


def half_kernel(
    edge_a, edge_b, state, history, rates, quadratic, precond, vel,
    strips, send_a, send_b,
    state_ring, state_ring_s, damp_ref, damp_s, v_ref, v_s, ring, ring_s, *, counts,
):
    count, rows, _ = state.shape
    cols, flip = counts
    tiles = rows // 8
    low = lane_of(rows) % 8 < 4
    odd = odd_part(flip) == 1
    position = lax.axis_index("col")
    has_left = (position > 0).astype(F32)
    has_right = (position < cols - 1).astype(F32)
    for pair in range(count + 2):
        a, b = edge_a[pair], edge_b[pair]
        left = a * has_left
        right = b * has_right
        strips[2 * pair] = jnp.where(low, right, left)
        strips[2 * pair + 1] = jnp.where(low, roll_lanes(right, -4), roll_lanes(left, 4))

    speed = speeds(vel, count)
    for n in range(tiles):
        for s in range(count):
            state_ring.at[s][tile_rows(n), :] = state[s, tile_rows(n), :]
        state_ring_s[tile_rows(n), :] = strips[2 * count, tile_rows(n), :]

    def putter(main, strip, n):
        def put(s, value):
            if s is None:
                strip[tile_rows(n), :] = value
            else:
                main[s, tile_rows(n), :] = value

        return put

    def getter(main, strip, n):
        return lambda s: strip[tile_rows(n), :] if s is None else main[s, tile_rows(n), :]

    def condition(k):
        for n in range(tiles):
            v = [v_ref[s, tile_rows(n), :] for s in range(count)]
            z = products(lambda s, t: precond[s, t, tile_rows(n), :], v)
            for s in range(count):
                ring.at[k, s][tile_rows(n), :] = z[s]
            z_s = strip_product(strips, count, n, v_s[tile_rows(n), :], count)
            ring_s.at[k][tile_rows(n), :] = z_s

    for n in range(tiles):
        first_vector(
            n, state_ring, state_ring_s,
            lambda s: quadratic[s, tile_rows(n), :], lambda s: history[s, tile_rows(n), :],
            lambda s, t: rates[s, t, tile_rows(n), :], strips, speed, count,
            putter(v_ref, v_s, n), putter(damp_ref, damp_s, n),
        )
    condition(0)
    for n in range(tiles):
        next_vector(
            n, ring.at[0], ring_s.at[0], getter(v_ref, v_s, n),
            lambda s, t: rates[s, t, tile_rows(n), :], strips, speed, count,
            putter(v_ref, v_s, n), getter(damp_ref, damp_s, n),
        )
    condition(1)

    single = [state.at[s] for s in range(count)]
    single += [ring.at[k, s] for k in range(2) for s in range(count)]
    single += [strips.at[2 * count]] + [ring_s.at[k] for k in range(2)]
    base = 2 * count + 4
    for target, (near, far) in zip((send_a, send_b), edge_rows(rows, flip)):
        for g in range(base):
            target[g] = strips[g, pl.ds(near, 2), :]
        for j, ref in enumerate(single):
            target[base + j // 2, pl.ds(j % 2, 1), :] = ref[pl.ds(far, 1), :]
        if len(single) % 2:
            target[base + len(single) // 2, pl.ds(1, 1), :] = jnp.zeros((1, LANES), F32)


def raw_planes(count):
    return 2 * count * count + 3 * count


def message_planes(count):
    return (2 * count + 4) + (3 * count + 3 + 1) // 2


def pairs_of(width):
    return [(i, j) for i in range(width) for j in range(i, width)]


def full_kernel(
    raw_a, raw_b, got_a, got_b, strips_in, state, history, rates, quadratic, precond, vel,
    z_out, gram_out,
    halo_rates, halo_precond, halo_fields, strips, inject_ref, inject_s,
    state_ring, state_ring_s, damp_ref, damp_s, v_ref, v_s, ring, ring_s,
    split_high, split_low, *, row_count, flip,
):
    count, rows, _ = state.shape
    own = rows // 8
    tiles = own + 1
    odd = odd_part(flip)
    position = lax.axis_index("row")
    above, below = position > 0, position < row_count - 1
    up_a = odd == 0
    keep_a = jnp.where(up_a, above, below).astype(F32)
    keep_b = jnp.where(up_a, below, above).astype(F32)
    near_a, far_a = 6 * (1 - odd), 5 * (1 - odd) + 2 * odd
    near_b, far_b = 6 * odd, 5 * odd + 2 * (1 - odd)
    raws = ((raw_a, near_a, keep_a), (raw_b, near_b, keep_b))
    lates = ((got_a, near_a, keep_a), (got_b, near_b, keep_b))
    blank = jnp.zeros((8, LANES), F32)

    def receive(target, at, sources, index, masked=False):
        for source, near, keep in sources:
            value = source[index]
            target[pl.ds(at + near, 2), :] = value * keep if masked else value

    base = 0
    for halo in (halo_rates, halo_precond):
        for k in range(count * count):
            receive(halo.at[k], 0, raws, base)
            base += 1
    for f in range(3):
        for s in range(count):
            halo_fields[f, s] = blank
            receive(halo_fields.at[f, s], 0, raws, base, f == 0)
            base += 1
    base = 2 * count + 4
    for g in range(base):
        strips[g, 0:rows, :] = strips_in[g]
        strips[g, rows : rows + 8, :] = blank
        receive(strips.at[g], rows, lates, g, g in (2 * count, 2 * count + 3))
    single = [halo_fields.at[0, s] for s in range(count)]
    for k in range(2):
        for s in range(count):
            inject_ref[k, s] = blank
            single.append(inject_ref.at[k, s])
    single.append(strips.at[2 * count, rows : rows + 8])
    for k in range(2):
        inject_s[k] = blank
        single.append(inject_s.at[k])
    for j, target in enumerate(single):
        for source, far, keep in ((got_a, far_a, keep_a), (got_b, far_b, keep_b)):
            row = source[base + j // 2, pl.ds(j % 2, 1), :]
            target[pl.ds(far, 1), :] = row * keep

    speed = speeds(vel, count)
    for n in range(tiles):
        for s in range(count):
            value = state[s, tile_rows(n), :] if n < own else halo_fields[0, s]
            state_ring.at[s][tile_rows(n), :] = value
        state_ring_s[tile_rows(n), :] = strips[2 * count, tile_rows(n), :]

    def putter(main, strip, n):
        def put(s, value):
            if s is None:
                strip[tile_rows(n), :] = value
            else:
                main[s, tile_rows(n), :] = value

        return put

    def getter(main, strip, n):
        return lambda s: strip[tile_rows(n), :] if s is None else main[s, tile_rows(n), :]

    def tile_of(block, halo, n):
        if n < own:
            return lambda s, t: block[s, t, tile_rows(n), :]
        return lambda s, t: halo[s * count + t]

    for n in range(tiles):
        plane = lambda ref, f: (
            (lambda s: ref[s, tile_rows(n), :]) if n < own else (lambda s: halo_fields[f, s])
        )
        first_vector(
            n, state_ring, state_ring_s, plane(quadratic, 1), plane(history, 2),
            tile_of(rates, halo_rates, n), strips, speed, count,
            putter(v_ref.at[0], v_s.at[0], n), putter(damp_ref, damp_s, n),
        )

    own_tiles = [(s, tile_rows(n)) for s in range(count) for n in range(own)]
    high, low, largest = {}, {}, []

    def gram_column(k):
        most = blank
        for s, at in own_tiles:
            value = v_ref[k, s, at, :]
            split_high[k, s, at, :], split_low[k, s, at, :] = split(value)
            most = jnp.maximum(most, jnp.abs(value))
        most = jnp.max(jnp.max(most, axis=0, keepdims=True), axis=1, keepdims=True)
        largest.append(jnp.broadcast_to(most, (8, LANES)))
        for i in range(k + 1):
            start = 64.0 * (largest[i] * largest[k])
            total, lost = start, blank
            for s, at in own_tiles:
                a = split_high[i, s, at, :]
                product = a * split_high[k, s, at, :]
                rest = a * split_low[k, s, at, :] + split_low[i, s, at, :] * v_ref[k, s, at, :]
                after = total + product
                lost = lost + ((product - (after - total)) + rest)
                total = after
            high[i, k], low[i, k] = total - start, lost

    gram_column(0)
    row = row_of(8)
    inside = ((row < 2) & below) | ((row > 5) & above)
    for k in range(KRYLOV):
        last = k == KRYLOV - 1
        pick = min(k, 1)
        for n in range(tiles):
            v = [v_ref[k, s, tile_rows(n), :] for s in range(count)]
            z = products(tile_of(precond, halo_precond, n), v)
            for s in range(count):
                if n < own:
                    z_out[k, s, tile_rows(n), :] = z[s]
                else:
                    z[s] = jnp.where(inside, z[s], inject_ref[pick, s])
                ring.at[s][tile_rows(n), :] = z[s]
            if n < own or not last:
                z_s = strip_product(strips, count, n, v_s[k, tile_rows(n), :], count)
                if n >= own:
                    z_s = jnp.where(inside, z_s, inject_s[pick])
                ring_s[tile_rows(n), :] = z_s
        for n in range(own if last else tiles):
            next_vector(
                n, ring, ring_s, getter(v_ref.at[k], v_s.at[k], n),
                tile_of(rates, halo_rates, n), strips, speed, count,
                putter(v_ref.at[k + 1], v_s.at[k + 1], n), getter(damp_ref, damp_s, n),
                not last,
            )
        gram_column(k + 1)

    row16, lane16 = row_of(16), lane_of(16)
    packs = [jnp.zeros((16, LANES), F32)] * 3
    for n, (i, j) in enumerate(pairs_of(KRYLOV + 1)):
        unit = largest[i] * largest[j]
        coarse, fine = 65536.0 * unit, 8.0 * unit
        first = (high[i, j] + coarse) - coarse
        rest = high[i, j] - first
        second = (rest + fine) - fine
        parts = [first, second, (rest - second) + low[i, j]]
        for shift in (4, 2, 1):
            parts = [x + roll_rows(x, shift) for x in parts]
        packs = [
            jnp.where(row16 == n, jnp.concatenate([x, x], axis=0), pack)
            for x, pack in zip(parts, packs)
        ]
    sums = [jnp.broadcast_to(jnp.sum(x, axis=1, keepdims=True), (16, LANES)) for x in packs]
    top, bottom = two_sum(sums[0], sums[1])
    top, bottom = quick_sum(top, bottom + sums[2])
    line = jnp.where(row16 == lane16, top, 0.0) + jnp.where(row16 + 16 == lane16, bottom, 0.0)
    line = line[:8] + line[8:]
    for shift in (4, 2, 1):
        line = line + roll_rows(line, shift)
    for r in range(0, gram_out.shape[0], 8):
        gram_out[r : r + 8, :] = line


def small_problem(gram):
    width = KRYLOV + 1
    work = dict(gram)
    unit = {}
    pivot = []
    for k in range(width):
        dh, dl = work[k, k]
        pivot.append(jnp.maximum(dh, 0.0))
        inverse = jnp.where(dh > 0.0, 1.0 / jnp.where(dh > 0.0, dh, 1.0), 0.0)
        factor = {}
        for i in range(k + 1, width):
            sh, sl = work[k, i]
            q = sh * inverse
            p, e = two_prod(q, dh)
            rest = ((sh - p) - e) + (sl - q * dl)
            factor[i] = quick_sum(q, rest * inverse)
            unit[k, i] = factor[i][0]
        for i in range(k + 1, width):
            for j in range(i, width):
                fh, fl = factor[i]
                sh, sl = work[k, j]
                p, e = two_prod(fh, sh)
                e = e + (fh * sl + fl * sh)
                wh, wl = work[i, j]
                h, error = two_sum(wh, -p)
                work[i, j] = quick_sum(h, error + (wl - e))
    norm = [jnp.sqrt(d) for d in pivot]
    back = [jnp.where(n > 0.0, 1.0 / jnp.where(n > 0.0, n, 1.0), 0.0) for n in norm]
    inv = {}
    for j in range(KRYLOV):
        inv[j, j] = back[j]
        for i in reversed(range(j)):
            total = unit[i, j] * back[j]
            for m in range(i + 1, j):
                total = total + unit[i, m] * inv[m, j]
            inv[i, j] = -total
    arnoldi = {}
    for j in range(KRYLOV):
        shifted = [inv[0, j]]
        for i in range(1, j + 1):
            shifted.append(inv[i, j] + inv[i - 1, j])
        shifted.append(inv[j, j])
        for i in range(j + 2):
            total = shifted[i]
            for m in range(i + 1, j + 2):
                total = total + unit[i, m] * shifted[m]
            arnoldi[i, j] = norm[i] * total
    beta = jnp.sqrt(pivot[0] + tiny_eps)
    basis = [[norm[0] / beta]]
    hessen = {}
    for k in range(KRYLOV):
        vector = []
        for i in range(k + 2):
            terms = [arnoldi[i, j] * basis[k][j] for j in range(max(i - 1, 0), k + 1)]
            vector.append(functools.reduce(jnp.add, terms))
        for i in range(k + 1):
            terms = [a * b for a, b in zip(basis[i], vector)]
            hessen[i, k] = functools.reduce(jnp.add, terms)
        for m in range(k + 1):
            terms = [hessen[i, k] * basis[i][m] for i in range(m, k + 1)]
            vector[m] = vector[m] - functools.reduce(jnp.add, terms)
        squared = functools.reduce(jnp.add, [x * x for x in vector])
        size = jnp.sqrt(squared + tiny_eps)
        hessen[k + 1, k] = size
        basis.append([x / size for x in vector])
    rotated = [beta] + [jnp.zeros_like(beta)] * KRYLOV
    for k in range(KRYLOV):
        first, second = hessen[k, k], hessen[k + 1, k]
        radius = jnp.sqrt(first * first + second * second)
        cosine, sine = first / radius, second / radius
        for j in range(k, KRYLOV):
            upper = hessen[k, j]
            under = hessen.get((k + 1, j))
            hessen[k, j] = cosine * upper + sine * under
            hessen[k + 1, j] = cosine * under - sine * upper
        rotated[k], rotated[k + 1] = (
            cosine * rotated[k] + sine * rotated[k + 1],
            cosine * rotated[k + 1] - sine * rotated[k],
        )
    coef = [None] * KRYLOV
    for k in reversed(range(KRYLOV)):
        total = rotated[k]
        for j in range(k + 1, KRYLOV):
            total = total - hessen[k, j] * coef[j]
        coef[k] = total / hessen[k, k]
    in_q = [
        functools.reduce(jnp.add, [coef[k] * basis[k][m] for k in range(m, KRYLOV)])
        for m in range(KRYLOV)
    ]
    in_v = [
        functools.reduce(jnp.add, [inv[i, j] * in_q[j] for j in range(i, KRYLOV)])
        for i in range(KRYLOV)
    ]
    return in_v, jnp.abs(rotated[KRYLOV])


def solve_kernel(gathered, z_ref, state, updated, residual):
    count, rows, _ = state.shape
    high = gathered[0:8, :]
    low = roll_lanes(high, -16)
    for r in range(8, gathered.shape[0], 8):
        tile = gathered[r : r + 8, :]
        high, error = two_sum(high, tile)
        low = low + roll_lanes(tile, -16) + error
    for shift in (4, 2, 1):
        high, error = two_sum(high, roll_rows(high, shift))
        low = low + roll_rows(low, shift) + error
    high, low = quick_sum(high, low)
    gram = {}
    for n, pair in enumerate(pairs_of(KRYLOV + 1)):
        gram[pair] = (
            jnp.broadcast_to(high[:, n : n + 1], (8, LANES)),
            jnp.broadcast_to(low[:, n : n + 1], (8, LANES)),
        )
    weights, last = small_problem(gram)
    for s in range(count):
        for r in range(0, rows, 8):
            total = weights[0] * z_ref[0, s, r : r + 8, :]
            for k in range(1, KRYLOV):
                total = total + weights[k] * z_ref[k, s, r : r + 8, :]
            updated[s, r : r + 8, :] = state[s, r : r + 8, :] + total
    residual[0] = last[0, 0]


def closed_chain(parts, size, flip):
    chain = []
    for p in range(parts):
        for r in range(size):
            if flip and p % 2:
                target = (p, r - 1) if r else (p - 1, 0)
            elif flip:
                target = (p, r + 1) if r < size - 1 else (p + 1, r)
            else:
                target = (p, (r + 1) % size)
            chain.append((p * size + r, target[0] * size + target[1]))
    return chain, [(b, a) for a, b in chain]


def shapes(*dims):
    return jax.ShapeDtypeStruct(dims, F32)


def body(state, history, rates, quadratic, velocity, precond):
    count, rows, _ = state.shape
    part_count = lax.axis_size("parts")
    row_count = lax.axis_size("row")
    col_count = lax.axis_size("col")
    flip = part_count % 2 == 0
    block = (count, rows, LANES)

    square = (count,) + block
    smem = pl.BlockSpec(memory_space=pltpu.SMEM)
    whole = pl.BlockSpec(memory_space=pltpu.VMEM)
    inputs = [
        pltpu.with_memory_space_constraint(x, pltpu.HBM)
        for x in (state, history, rates, quadratic, precond)
    ]
    (
        state, history, rates, quadratic, precond, edge_a, edge_b, send_a, send_b
    ) = pl.pallas_call(
        functools.partial(pack_kernel, flip=flip),
        in_specs=[pl.BlockSpec(memory_space=pltpu.HBM)] * 5,
        out_shape=[
            shapes(*block), shapes(*block), shapes(*square), shapes(*block), shapes(*square),
            shapes(count + 2, rows, LANES), shapes(count + 2, rows, LANES),
            shapes(raw_planes(count), 2, LANES), shapes(raw_planes(count), 2, LANES),
        ],
        out_specs=[whole] * 9,
        scratch_shapes=[pltpu.SemaphoreType.DMA((5,))],
        compiler_params=VMEM,
        name="pack_columns",
    )(*inputs)
    down, up = closed_chain(part_count, row_count, flip)
    right, left = closed_chain(part_count, col_count, False)
    got_a = lax.ppermute(edge_a, ("parts", "col"), right)
    got_b = lax.ppermute(edge_b, ("parts", "col"), left)
    raw_a = lax.ppermute(send_a, ("parts", "row"), down)
    raw_b = lax.ppermute(send_b, ("parts", "row"), up)

    planes = message_planes(count)
    strips, send_a, send_b = pl.pallas_call(
        functools.partial(half_kernel, counts=(col_count, flip)),
        in_specs=[whole] * 8,
        out_shape=[shapes(2 * count + 4, rows, LANES)] + [shapes(planes, 2, LANES)] * 2,
        scratch_shapes=[
            pltpu.VMEM((count, rows, LANES), F32),
            pltpu.VMEM((rows, LANES), F32),
            pltpu.VMEM(block, F32),
            pltpu.VMEM((rows, LANES), F32),
            pltpu.VMEM(block, F32),
            pltpu.VMEM((rows, LANES), F32),
            pltpu.VMEM((2, count, rows, LANES), F32),
            pltpu.VMEM((2, rows, LANES), F32),
        ],
        compiler_params=VMEM,
        name="half_step",
    )(got_a, got_b, state, history, rates, quadratic, precond, velocity)

    got_a = lax.ppermute(send_a, ("parts", "row"), down)
    got_b = lax.ppermute(send_b, ("parts", "row"), up)

    ext = rows + 8
    members = row_count * col_count
    z, gram = pl.pallas_call(
        functools.partial(full_kernel, row_count=row_count, flip=flip),
        in_specs=[whole] * 11,
        out_shape=[shapes(KRYLOV, *block), shapes(members, LANES)],
        scratch_shapes=[
            pltpu.VMEM((count * count, 8, LANES), F32),
            pltpu.VMEM((count * count, 8, LANES), F32),
            pltpu.VMEM((3, count, 8, LANES), F32),
            pltpu.VMEM((2 * count + 4, ext, LANES), F32),
            pltpu.VMEM((2, count, 8, LANES), F32),
            pltpu.VMEM((2, 8, LANES), F32),
            pltpu.VMEM((count, ext, LANES), F32),
            pltpu.VMEM((ext, LANES), F32),
            pltpu.VMEM((count, ext, LANES), F32),
            pltpu.VMEM((ext, LANES), F32),
            pltpu.VMEM((KRYLOV + 1, count, ext, LANES), F32),
            pltpu.VMEM((KRYLOV + 1, ext, LANES), F32),
            pltpu.VMEM((count, ext, LANES), F32),
            pltpu.VMEM((ext, LANES), F32),
            pltpu.VMEM((KRYLOV + 1,) + block, F32),
            pltpu.VMEM((KRYLOV + 1,) + block, F32),
        ],
        compiler_params=VMEM,
        name="krylov",
    )(raw_a, raw_b, got_a, got_b, strips, state, history, rates, quadratic, precond, velocity)

    gathered = lax.all_to_all(gram, ("row", "col"), 0, 0, tiled=True)
    updated, last = pl.pallas_call(
        solve_kernel,
        out_shape=[shapes(*block), shapes(1)],
        out_specs=[whole, smem],
        compiler_params=VMEM,
        name="solve",
    )(gathered, z, state)
    return updated, last


def solution(mesh):
    placed = (
        P(None, ("parts", "row"), "col"),
        P(None, ("parts", "row"), "col"),
        P(None, None, ("parts", "row"), "col"),
        P(None, ("parts", "row"), "col"),
        P(),
        P(None, None, ("parts", "row"), "col"),
    )
    return jax.shard_map(
        body,
        mesh=mesh,
        in_specs=placed,
        out_specs=(P(None, ("parts", "row"), "col"), P("parts")),
        check_vma=False,
    )
```

```python
import functools

import jax
import jax.numpy as jnp
from jax import lax
from jax.experimental import pallas as pl
from jax.experimental.pallas import tpu as pltpu
from jax.sharding import PartitionSpec as P

KRYLOV = 4
step_gamma = 0.4
tiny_eps = 1e-12

F32 = jnp.float32
LANES = 128
VMEM = pltpu.CompilerParams(vmem_limit_bytes=48 * 1024 * 1024)


def lane_of(rows):
    return lax.broadcasted_iota(jnp.int32, (rows, LANES), 1)


def row_of(rows):
    return lax.broadcasted_iota(jnp.int32, (rows, LANES), 0)


def roll_lanes(x, shift):
    shift %= LANES
    return pltpu.roll(x, shift, 1) if shift else x


def roll_rows(x, shift):
    return pltpu.roll(x, shift % x.shape[0], 0)


def slot_of(rows):
    return ((131 - lane_of(rows)) // 8) % 16


def two_sum(a, b):
    s = a + b
    t = s - a
    return s, (a - (s - t)) + (b - t)


def quick_sum(a, b):
    s = a + b
    return s, b - (s - a)


def split(a):
    c = a * 4097.0
    high = c - (c - a)
    return high, a - high


def two_prod(a, b):
    p = a * b
    ah, al = split(a)
    bh, bl = split(b)
    return p, ((ah * bh - p) + ah * bl + al * bh) + al * bl


def tile_rows(n):
    return slice(8 * n, 8 * n + 8)


def vertical(field, n):
    tiles = field.shape[0] // 8
    this = field[tile_rows(n), :]
    following = field[tile_rows((n + 1) % tiles), :]
    leading = field[tile_rows((n - 1) % tiles), :]
    row = row_of(8)
    under = roll_rows(jnp.where(row == 0, following, this), -1)
    over = roll_rows(jnp.where(row == 7, leading, this), 1)
    return under - over


def speeds(vel, count):
    slot = slot_of(8)
    mains = [
        tuple(
            jnp.broadcast_to(0.5 * step_gamma * vel[s : s + 1, d : d + 1], (8, LANES))
            for d in range(2)
        )
        for s in range(count)
    ]
    strip = [jnp.zeros((8, LANES), F32)] * 2
    for s in range(count):
        strip = [jnp.where(slot == s, x, y) for x, y in zip(mains[s], strip)]
    return mains, strip


def diagonals(count):
    return range(-((count - 1) // 2), count // 2 + 1)


def sum_of(terms):
    return functools.reduce(jnp.add, terms)


def products(tile, fields):
    span = range(len(fields))
    return [sum_of([tile(s, t) * fields[t] for t in span]) for s in span]


def strip_product(strips, base, n, strip, count):
    slot = slot_of(8)
    past_end = jnp.where(slot < count, strip, roll_lanes(strip, -8 * count))
    past_start = jnp.where(slot < count, strip, roll_lanes(strip, -8 * (16 - count)))
    return sum_of(
        [
            strips[base + g, tile_rows(n), :] * roll_lanes(past_end if d >= 0 else past_start, 8 * d)
            for g, d in enumerate(diagonals(count))
        ]
    )


def drift(ring, ring_s, n, speed, count, second=None, with_strip=True):
    vel, vel_s = speed
    lane, slot = lane_of(8), slot_of(8)
    strip = ring_s[tile_rows(n), :]
    edge = jnp.zeros((8, LANES), F32)
    mains, moved = [], []
    for s in range(count):
        main = ring[s, tile_rows(n), :]
        outer = roll_lanes(strip, 8 * s)
        left = roll_lanes(jnp.where(lane == LANES - 1, outer, main), 1)
        right = roll_lanes(jnp.where(lane == 0, outer, main), -1)
        along_x = vertical(ring.at[s], n)
        moved.append(vel[s][0] * along_x + vel[s][1] * (right - left))
        if with_strip:
            edge = jnp.where(slot == s, roll_lanes(main, -8 * s), edge)
        mains.append(main)
    if not with_strip:
        return mains, strip, moved, None
    left = roll_lanes(jnp.where(lane % 8 == 7, edge, strip), 1)
    right = roll_lanes(jnp.where(lane % 8 == 0, edge, strip), -1)
    if second is not None:
        left = jnp.where(lane % 8 == 4, roll_lanes(second, -3), left)
        right = jnp.where(lane % 8 == 3, roll_lanes(second, 3), right)
    along_x = vertical(ring_s, n)
    return mains, strip, moved, vel_s[0] * along_x + vel_s[1] * (right - left)


def first_vector(n, state_ring, state_ring_s, quad, hist, rates, strips, speed, count, put, damp):
    base = 2 * count
    second = strips[base + 3, tile_rows(n), :]
    state, strip, moved, moved_s = drift(state_ring, state_ring_s, n, speed, count, second)
    linear = products(rates, state)
    for s in range(count):
        loss = step_gamma * quad(s) * state[s]
        damp(s, 1.0 + 2.0 * loss)
        put(s, ((hist(s) - state[s]) - moved[s]) + (step_gamma * linear[s] - loss * state[s]))
    linear = strip_product(strips, 0, n, strip, count)
    loss = step_gamma * strips[base + 1, tile_rows(n), :] * strip
    damp(None, 1.0 + 2.0 * loss)
    past = strips[base + 2, tile_rows(n), :]
    put(None, ((past - strip) - moved_s) + (step_gamma * linear - loss * strip))


def next_vector(n, ring, ring_s, old, rates, strips, speed, count, put, damp, with_strip=True):
    z, strip, moved, moved_s = drift(ring, ring_s, n, speed, count, None, with_strip)
    linear = products(rates, z)
    for s in range(count):
        put(s, ((damp(s) * z[s] - old(s)) + moved[s]) - step_gamma * linear[s])
    if with_strip:
        linear = strip_product(strips, 0, n, strip, count)
        put(None, ((damp(None) * strip - old(None)) + moved_s) - step_gamma * linear)


def odd_place(axis):
    return lax.axis_index(axis) % 2


def edge_rows(rows):
    odd = odd_place("row")
    down, up = (rows - 2, rows - 3), (0, 2)
    return tuple(
        tuple(x + (y - x) * odd for x, y in zip(*ends)) for ends in ((down, up), (up, down))
    )


def pack_kernel(
    state_in, history_in, rates_in, quadratic_in, precond_in,
    state, history, rates, quadratic, precond, edge_a, edge_b, raw_a, raw_b, sems,
):
    count, rows, _ = state.shape
    copies = [
        pltpu.make_async_copy(source, target, sems.at[n])
        for n, (source, target) in enumerate(
            (
                (rates_in, rates),
                (precond_in, precond),
                (state_in, state),
                (quadratic_in, quadratic),
                (history_in, history),
            )
        )
    ]
    for copy in copies:
        copy.start()
    odd = odd_place("col") == 1
    slot = slot_of(rows)
    low = lane_of(rows) % 8 < 4

    def place(group, s, at):
        if group < 2 * count:
            other = (s + diagonals(count)[group % count]) % count
            return roll_lanes((rates if group < count else precond)[s, other], -8 * at)
        plane = (state, quadratic, history, state)[group - 2 * count][s]
        if group < 2 * count + 3:
            return roll_lanes(plane, -8 * at)
        return jnp.where(low, roll_lanes(plane, -4 - 8 * at), roll_lanes(plane, 4 - 8 * at))

    def fill(planes):
        packed = jnp.zeros((rows, LANES), F32)
        for at, (group, s) in enumerate(planes):
            packed = jnp.where(slot == at, place(group, s, at), packed)
        return packed

    done = set()
    spare = 16 - count
    for pair in range(strip_pairs(count)):
        first, second, third = (3 * pair + n for n in range(3))
        ready = 1 if third < count else 2 if third < 2 * count else 5
        for n in range(ready):
            if n not in done:
                copies[n].wait()
                done.add(n)
        species = range(count)
        one = fill([(first, s) for s in species] + [(third, s) for s in species[:spare]])
        two = fill([(second, s) for s in species] + [(third, s) for s in species[spare:]])
        right = jnp.where(low, roll_lanes(two, -4), one)
        left = jnp.where(low, one, roll_lanes(two, 4))
        edge_a[pair] = jnp.where(odd, left, right)
        edge_b[pair] = jnp.where(odd, right, left)

    for target, (near, _) in zip((raw_a, raw_b), edge_rows(rows)):
        planes = [m.at[s, t] for m in (rates, precond) for s in range(count) for t in range(count)]
        planes += [ref.at[s] for ref in (state, quadratic, history) for s in range(count)]
        for n, ref in enumerate(planes):
            target[n] = ref[pl.ds(near, 2), :]


def half_kernel(
    edge_a, edge_b, state, history, rates, quadratic, precond, vel,
    strips, send_a, send_b,
    state_ring, state_ring_s, damp_ref, damp_s, v_ref, v_s, ring, ring_s, *, cols,
):
    count, rows, _ = state.shape
    tiles = rows // 8
    low = lane_of(rows) % 8 < 4
    odd = odd_place("col") == 1
    position = lax.axis_index("col")
    has_left = (position > 0).astype(F32)
    has_right = (position < cols - 1).astype(F32)
    spare = slot_of(rows) < 16 - count
    for pair in range(strip_pairs(count)):
        a, b = edge_a[pair], edge_b[pair]
        left = jnp.where(odd, a, b) * has_left
        right = jnp.where(odd, b, a) * has_right
        one = jnp.where(low, right, left)
        two = jnp.where(low, roll_lanes(right, -4), roll_lanes(left, 4))
        strips[3 * pair] = one
        strips[3 * pair + 1] = two
        strips[3 * pair + 2] = jnp.where(
            spare, roll_lanes(one, 8 * count), roll_lanes(two, 8 * (2 * count - 16))
        )

    speed = speeds(vel, count)
    for n in range(tiles):
        for s in range(count):
            state_ring.at[s][tile_rows(n), :] = state[s, tile_rows(n), :]
        state_ring_s[tile_rows(n), :] = strips[2 * count, tile_rows(n), :]

    def putter(main, strip, n):
        def put(s, value):
            if s is None:
                strip[tile_rows(n), :] = value
            else:
                main[s, tile_rows(n), :] = value

        return put

    def getter(main, strip, n):
        return lambda s: strip[tile_rows(n), :] if s is None else main[s, tile_rows(n), :]

    def condition(k):
        for n in range(tiles):
            v = [v_ref[s, tile_rows(n), :] for s in range(count)]
            z = products(lambda s, t: precond[s, t, tile_rows(n), :], v)
            for s in range(count):
                ring.at[k, s][tile_rows(n), :] = z[s]
            z_s = strip_product(strips, count, n, v_s[tile_rows(n), :], count)
            ring_s.at[k][tile_rows(n), :] = z_s

    for n in range(tiles):
        first_vector(
            n, state_ring, state_ring_s,
            lambda s: quadratic[s, tile_rows(n), :], lambda s: history[s, tile_rows(n), :],
            lambda s, t: rates[s, t, tile_rows(n), :], strips, speed, count,
            putter(v_ref, v_s, n), putter(damp_ref, damp_s, n),
        )
    condition(0)
    for n in range(tiles):
        next_vector(
            n, ring.at[0], ring_s.at[0], getter(v_ref, v_s, n),
            lambda s, t: rates[s, t, tile_rows(n), :], strips, speed, count,
            putter(v_ref, v_s, n), getter(damp_ref, damp_s, n),
        )
    condition(1)

    single = [state.at[s] for s in range(count)]
    single += [ring.at[k, s] for k in range(2) for s in range(count)]
    single += [strips.at[2 * count]] + [ring_s.at[k] for k in range(2)]
    base = 2 * count + 4
    for target, (near, far) in zip((send_a, send_b), edge_rows(rows)):
        for g in range(base):
            target[g] = strips[g, pl.ds(near, 2), :]
        for j, ref in enumerate(single):
            target[base + j // 2, pl.ds(j % 2, 1), :] = ref[pl.ds(far, 1), :]
        if len(single) % 2:
            target[base + len(single) // 2, pl.ds(1, 1), :] = jnp.zeros((1, LANES), F32)


def strip_pairs(count):
    return (2 * count + 4) // 3


def raw_planes(count):
    return 2 * count * count + 3 * count


def message_planes(count):
    return (2 * count + 4) + (3 * count + 3 + 1) // 2


def pairs_of(width):
    return [(i, j) for i in range(width) for j in range(i, width)]


def full_kernel(
    raw_a, raw_b, got_a, got_b, strips_in, state, history, rates, quadratic, precond, vel,
    z_out, gram_out,
    halo_rates, halo_precond, halo_fields, strips, inject_ref, inject_s,
    state_ring, state_ring_s, damp_ref, damp_s, v_ref, v_s, ring, ring_s,
    split_high, split_low, *, row_count,
):
    count, rows, _ = state.shape
    own = rows // 8
    tiles = own + 1
    odd = odd_place("row")
    position = lax.axis_index("row")
    above, below = position > 0, position < row_count - 1
    keep_a = jnp.where(odd == 1, above, below).astype(F32)
    keep_b = jnp.where(odd == 1, below, above).astype(F32)
    near_a, far_a = 6 * odd, 5 * odd + 2 * (1 - odd)
    near_b, far_b = 6 * (1 - odd), 5 * (1 - odd) + 2 * odd
    raws = ((raw_a, near_a, keep_a), (raw_b, near_b, keep_b))
    lates = ((got_a, near_a, keep_a), (got_b, near_b, keep_b))
    blank = jnp.zeros((8, LANES), F32)

    def receive(target, at, sources, index, masked=False):
        for source, near, keep in sources:
            value = source[index]
            target[pl.ds(at + near, 2), :] = value * keep if masked else value

    base = 0
    for halo in (halo_rates, halo_precond):
        for k in range(count * count):
            receive(halo.at[k], 0, raws, base)
            base += 1
    for f in range(3):
        for s in range(count):
            halo_fields[f, s] = blank
            receive(halo_fields.at[f, s], 0, raws, base, f == 0)
            base += 1
    base = 2 * count + 4
    for g in range(base):
        strips[g, 0:rows, :] = strips_in[g]
        strips[g, rows : rows + 8, :] = blank
        receive(strips.at[g], rows, lates, g, g in (2 * count, 2 * count + 3))
    single = [halo_fields.at[0, s] for s in range(count)]
    for k in range(2):
        for s in range(count):
            inject_ref[k, s] = blank
            single.append(inject_ref.at[k, s])
    single.append(strips.at[2 * count, rows : rows + 8])
    for k in range(2):
        inject_s[k] = blank
        single.append(inject_s.at[k])
    for j, target in enumerate(single):
        for source, far, keep in ((got_a, far_a, keep_a), (got_b, far_b, keep_b)):
            row = source[base + j // 2, pl.ds(j % 2, 1), :]
            target[pl.ds(far, 1), :] = row * keep

    speed = speeds(vel, count)
    for n in range(tiles):
        for s in range(count):
            value = state[s, tile_rows(n), :] if n < own else halo_fields[0, s]
            state_ring.at[s][tile_rows(n), :] = value
        state_ring_s[tile_rows(n), :] = strips[2 * count, tile_rows(n), :]

    def putter(main, strip, n):
        def put(s, value):
            if s is None:
                strip[tile_rows(n), :] = value
            else:
                main[s, tile_rows(n), :] = value

        return put

    def getter(main, strip, n):
        return lambda s: strip[tile_rows(n), :] if s is None else main[s, tile_rows(n), :]

    def tile_of(block, halo, n):
        if n < own:
            return lambda s, t: block[s, t, tile_rows(n), :]
        return lambda s, t: halo[s * count + t]

    for n in range(tiles):
        plane = lambda ref, f: (
            (lambda s: ref[s, tile_rows(n), :]) if n < own else (lambda s: halo_fields[f, s])
        )
        first_vector(
            n, state_ring, state_ring_s, plane(quadratic, 1), plane(history, 2),
            tile_of(rates, halo_rates, n), strips, speed, count,
            putter(v_ref.at[0], v_s.at[0], n), putter(damp_ref, damp_s, n),
        )

    own_tiles = [(s, tile_rows(n)) for s in range(count) for n in range(own)]
    high, low, largest = {}, {}, []

    def gram_column(k):
        most = blank
        for s, at in own_tiles:
            value = v_ref[k, s, at, :]
            split_high[k, s, at, :], split_low[k, s, at, :] = split(value)
            most = jnp.maximum(most, jnp.abs(value))
        most = jnp.max(jnp.max(most, axis=0, keepdims=True), axis=1, keepdims=True)
        largest.append(jnp.broadcast_to(most, (8, LANES)))
        for i in range(k + 1):
            start = 64.0 * (largest[i] * largest[k])
            total, lost = start, blank
            for s, at in own_tiles:
                a = split_high[i, s, at, :]
                product = a * split_high[k, s, at, :]
                rest = a * split_low[k, s, at, :] + split_low[i, s, at, :] * v_ref[k, s, at, :]
                after = total + product
                lost = lost + ((product - (after - total)) + rest)
                total = after
            high[i, k], low[i, k] = total - start, lost

    gram_column(0)
    row = row_of(8)
    inside = ((row < 2) & below) | ((row > 5) & above)
    for k in range(KRYLOV):
        last = k == KRYLOV - 1
        pick = min(k, 1)
        for n in range(tiles):
            v = [v_ref[k, s, tile_rows(n), :] for s in range(count)]
            z = products(tile_of(precond, halo_precond, n), v)
            for s in range(count):
                if n < own:
                    z_out[k, s, tile_rows(n), :] = z[s]
                else:
                    z[s] = jnp.where(inside, z[s], inject_ref[pick, s])
                ring.at[s][tile_rows(n), :] = z[s]
            if n < own or not last:
                z_s = strip_product(strips, count, n, v_s[k, tile_rows(n), :], count)
                if n >= own:
                    z_s = jnp.where(inside, z_s, inject_s[pick])
                ring_s[tile_rows(n), :] = z_s
        for n in range(own if last else tiles):
            next_vector(
                n, ring, ring_s, getter(v_ref.at[k], v_s.at[k], n),
                tile_of(rates, halo_rates, n), strips, speed, count,
                putter(v_ref.at[k + 1], v_s.at[k + 1], n), getter(damp_ref, damp_s, n),
                not last,
            )
        gram_column(k + 1)

    row16, lane16 = row_of(16), lane_of(16)
    packs = [jnp.zeros((16, LANES), F32)] * 3
    for n, (i, j) in enumerate(pairs_of(KRYLOV + 1)):
        unit = largest[i] * largest[j]
        coarse, fine = 65536.0 * unit, 8.0 * unit
        first = (high[i, j] + coarse) - coarse
        rest = high[i, j] - first
        second = (rest + fine) - fine
        parts = [first, second, (rest - second) + low[i, j]]
        for shift in (4, 2, 1):
            parts = [x + roll_rows(x, shift) for x in parts]
        packs = [
            jnp.where(row16 == n, jnp.concatenate([x, x], axis=0), pack)
            for x, pack in zip(parts, packs)
        ]
    sums = [jnp.broadcast_to(jnp.sum(x, axis=1, keepdims=True), (16, LANES)) for x in packs]
    top, bottom = two_sum(sums[0], sums[1])
    top, bottom = quick_sum(top, bottom + sums[2])
    line = jnp.where(row16 == lane16, top, 0.0) + jnp.where(row16 + 16 == lane16, bottom, 0.0)
    line = line[:8] + line[8:]
    for shift in (4, 2, 1):
        line = line + roll_rows(line, shift)
    for r in range(0, gram_out.shape[0], 8):
        gram_out[r : r + 8, :] = line


def small_problem(gram):
    width = KRYLOV + 1
    work = dict(gram)
    unit = {}
    pivot = []
    for k in range(width):
        dh, dl = work[k, k]
        pivot.append(jnp.maximum(dh, 0.0))
        inverse = jnp.where(dh > 0.0, 1.0 / jnp.where(dh > 0.0, dh, 1.0), 0.0)
        factor = {}
        for i in range(k + 1, width):
            sh, sl = work[k, i]
            q = sh * inverse
            p, e = two_prod(q, dh)
            rest = ((sh - p) - e) + (sl - q * dl)
            factor[i] = quick_sum(q, rest * inverse)
            unit[k, i] = factor[i][0]
        for i in range(k + 1, width):
            for j in range(i, width):
                fh, fl = factor[i]
                sh, sl = work[k, j]
                p, e = two_prod(fh, sh)
                e = e + (fh * sl + fl * sh)
                wh, wl = work[i, j]
                h, error = two_sum(wh, -p)
                work[i, j] = quick_sum(h, error + (wl - e))
    norm = [jnp.sqrt(d) for d in pivot]
    back = [jnp.where(n > 0.0, 1.0 / jnp.where(n > 0.0, n, 1.0), 0.0) for n in norm]
    inv = {}
    for j in range(KRYLOV):
        inv[j, j] = back[j]
        for i in reversed(range(j)):
            total = unit[i, j] * back[j]
            for m in range(i + 1, j):
                total = total + unit[i, m] * inv[m, j]
            inv[i, j] = -total
    arnoldi = {}
    for j in range(KRYLOV):
        shifted = [inv[0, j]]
        for i in range(1, j + 1):
            shifted.append(inv[i, j] + inv[i - 1, j])
        shifted.append(inv[j, j])
        for i in range(j + 2):
            total = shifted[i]
            for m in range(i + 1, j + 2):
                total = total + unit[i, m] * shifted[m]
            arnoldi[i, j] = norm[i] * total
    beta = jnp.sqrt(pivot[0] + tiny_eps)
    basis = [[norm[0] / beta]]
    hessen = {}
    for k in range(KRYLOV):
        vector = []
        for i in range(k + 2):
            terms = [arnoldi[i, j] * basis[k][j] for j in range(max(i - 1, 0), k + 1)]
            vector.append(functools.reduce(jnp.add, terms))
        for i in range(k + 1):
            terms = [a * b for a, b in zip(basis[i], vector)]
            hessen[i, k] = functools.reduce(jnp.add, terms)
        for m in range(k + 1):
            terms = [hessen[i, k] * basis[i][m] for i in range(m, k + 1)]
            vector[m] = vector[m] - functools.reduce(jnp.add, terms)
        squared = functools.reduce(jnp.add, [x * x for x in vector])
        size = jnp.sqrt(squared + tiny_eps)
        hessen[k + 1, k] = size
        basis.append([x / size for x in vector])
    rotated = [beta] + [jnp.zeros_like(beta)] * KRYLOV
    for k in range(KRYLOV):
        first, second = hessen[k, k], hessen[k + 1, k]
        radius = jnp.sqrt(first * first + second * second)
        cosine, sine = first / radius, second / radius
        for j in range(k, KRYLOV):
            upper = hessen[k, j]
            under = hessen.get((k + 1, j))
            hessen[k, j] = cosine * upper + sine * under
            hessen[k + 1, j] = cosine * under - sine * upper
        rotated[k], rotated[k + 1] = (
            cosine * rotated[k] + sine * rotated[k + 1],
            cosine * rotated[k + 1] - sine * rotated[k],
        )
    coef = [None] * KRYLOV
    for k in reversed(range(KRYLOV)):
        total = rotated[k]
        for j in range(k + 1, KRYLOV):
            total = total - hessen[k, j] * coef[j]
        coef[k] = total / hessen[k, k]
    in_q = [
        functools.reduce(jnp.add, [coef[k] * basis[k][m] for k in range(m, KRYLOV)])
        for m in range(KRYLOV)
    ]
    in_v = [
        functools.reduce(jnp.add, [inv[i, j] * in_q[j] for j in range(i, KRYLOV)])
        for i in range(KRYLOV)
    ]
    return in_v, jnp.abs(rotated[KRYLOV])


def solve_kernel(gathered, z_ref, state, updated, residual):
    count, rows, _ = state.shape
    high = gathered[0:8, :]
    low = roll_lanes(high, -16)
    for r in range(8, gathered.shape[0], 8):
        tile = gathered[r : r + 8, :]
        high, error = two_sum(high, tile)
        low = low + roll_lanes(tile, -16) + error
    for shift in (4, 2, 1):
        high, error = two_sum(high, roll_rows(high, shift))
        low = low + roll_rows(low, shift) + error
    high, low = quick_sum(high, low)
    gram = {}
    for n, pair in enumerate(pairs_of(KRYLOV + 1)):
        gram[pair] = (
            jnp.broadcast_to(high[:, n : n + 1], (8, LANES)),
            jnp.broadcast_to(low[:, n : n + 1], (8, LANES)),
        )
    weights, last = small_problem(gram)
    for s in range(count):
        for r in range(0, rows, 8):
            total = weights[0] * z_ref[0, s, r : r + 8, :]
            for k in range(1, KRYLOV):
                total = total + weights[k] * z_ref[k, s, r : r + 8, :]
            updated[s, r : r + 8, :] = state[s, r : r + 8, :] + total
    residual[0] = last[0, 0]


def exchanges(parts, size):
    def pairing(start):
        out = []
        for p in range(parts):
            for r in range(size):
                mate = start + ((r - start) ^ 1) if r >= start else size
                other = (p, mate) if mate < size else (p if parts % 2 else p ^ 1, r)
                out.append((p * size + r, other[0] * size + other[1]))
        return out

    return pairing(0), pairing(1)


def ring_exchanges(size):
    if size % 2:
        return exchanges(1, size)
    pairs = [(r, r ^ 1) for r in range(size)]
    return pairs, [((a + 1) % size, (b + 1) % size) for a, b in pairs]


def shapes(*dims):
    return jax.ShapeDtypeStruct(dims, F32)


def body(state, history, rates, quadratic, velocity, precond):
    count, rows, _ = state.shape
    row_count = lax.axis_size("row")
    col_count = lax.axis_size("col")
    block = (count, rows, LANES)

    square = (count,) + block
    smem = pl.BlockSpec(memory_space=pltpu.SMEM)
    whole = pl.BlockSpec(memory_space=pltpu.VMEM)
    inputs = [
        pltpu.with_memory_space_constraint(x, pltpu.HBM)
        for x in (state, history, rates, quadratic, precond)
    ]
    (
        state, history, rates, quadratic, precond, edge_a, edge_b, send_a, send_b
    ) = pl.pallas_call(
        pack_kernel,
        in_specs=[pl.BlockSpec(memory_space=pltpu.HBM)] * 5,
        out_shape=[
            shapes(*block), shapes(*block), shapes(*square), shapes(*block), shapes(*square),
            shapes(strip_pairs(count), rows, LANES), shapes(strip_pairs(count), rows, LANES),
            shapes(raw_planes(count), 2, LANES), shapes(raw_planes(count), 2, LANES),
        ],
        out_specs=[whole] * 9,
        scratch_shapes=[pltpu.SemaphoreType.DMA((5,))],
        compiler_params=VMEM,
        name="pack_columns",
    )(*inputs)
    row_a, row_b = exchanges(lax.axis_size("parts"), row_count)
    col_a, col_b = ring_exchanges(col_count)
    got_a = lax.ppermute(edge_a, "col", col_a)
    got_b = lax.ppermute(edge_b, "col", col_b)
    raw_a = lax.ppermute(send_a, ("parts", "row"), row_a)
    raw_b = lax.ppermute(send_b, ("parts", "row"), row_b)

    planes = message_planes(count)
    strips, send_a, send_b = pl.pallas_call(
        functools.partial(half_kernel, cols=col_count),
        in_specs=[whole] * 8,
        out_shape=[shapes(2 * count + 4, rows, LANES)] + [shapes(planes, 2, LANES)] * 2,
        scratch_shapes=[
            pltpu.VMEM((count, rows, LANES), F32),
            pltpu.VMEM((rows, LANES), F32),
            pltpu.VMEM(block, F32),
            pltpu.VMEM((rows, LANES), F32),
            pltpu.VMEM(block, F32),
            pltpu.VMEM((rows, LANES), F32),
            pltpu.VMEM((2, count, rows, LANES), F32),
            pltpu.VMEM((2, rows, LANES), F32),
        ],
        compiler_params=VMEM,
        name="half_step",
    )(got_a, got_b, state, history, rates, quadratic, precond, velocity)

    got_b = lax.ppermute(send_b, ("parts", "row"), row_b)
    got_a = lax.ppermute(send_a, ("parts", "row"), row_a)

    ext = rows + 8
    members = row_count * col_count
    z, gram = pl.pallas_call(
        functools.partial(full_kernel, row_count=row_count),
        in_specs=[whole] * 11,
        out_shape=[shapes(KRYLOV, *block), shapes(members, LANES)],
        scratch_shapes=[
            pltpu.VMEM((count * count, 8, LANES), F32),
            pltpu.VMEM((count * count, 8, LANES), F32),
            pltpu.VMEM((3, count, 8, LANES), F32),
            pltpu.VMEM((2 * count + 4, ext, LANES), F32),
            pltpu.VMEM((2, count, 8, LANES), F32),
            pltpu.VMEM((2, 8, LANES), F32),
            pltpu.VMEM((count, ext, LANES), F32),
            pltpu.VMEM((ext, LANES), F32),
            pltpu.VMEM((count, ext, LANES), F32),
            pltpu.VMEM((ext, LANES), F32),
            pltpu.VMEM((KRYLOV + 1, count, ext, LANES), F32),
            pltpu.VMEM((KRYLOV + 1, ext, LANES), F32),
            pltpu.VMEM((count, ext, LANES), F32),
            pltpu.VMEM((ext, LANES), F32),
            pltpu.VMEM((KRYLOV + 1,) + block, F32),
            pltpu.VMEM((KRYLOV + 1,) + block, F32),
        ],
        compiler_params=VMEM,
        name="krylov",
    )(raw_a, raw_b, got_a, got_b, strips, state, history, rates, quadratic, precond, velocity)

    gathered = lax.all_to_all(gram, ("row", "col"), 0, 0, tiled=True)
    updated, last = pl.pallas_call(
        solve_kernel,
        out_shape=[shapes(*block), shapes(1)],
        out_specs=[whole, smem],
        compiler_params=VMEM,
        name="solve",
    )(gathered, z, state)
    return updated, last


def solution(mesh):
    placed = (
        P(None, ("parts", "row"), "col"),
        P(None, ("parts", "row"), "col"),
        P(None, None, ("parts", "row"), "col"),
        P(None, ("parts", "row"), "col"),
        P(),
        P(None, None, ("parts", "row"), "col"),
    )
    return jax.shard_map(
        body,
        mesh=mesh,
        in_specs=placed,
        out_specs=(P(None, ("parts", "row"), "col"), P("parts")),
        check_vma=False,
    )
```
